512 devices in a mesh: grp: 2 (over y), row: 16 (over z), col: 8 (over x), sub: 2 (over core).
Axes of the slice: x: 8, y: 2, z: 16, core: 2. Of those that a mesh axis runs over, the one named last changes fastest.
The devices are a block of a 8x16x16 slice.
Arguments:
- pair: bfloat16 [768, 384, 128], P(('grp', 'row'), ('col', 'sub')), parts along dimension 0, may hold values from -6 to 6
- chain_ids: int32 [768], P('grp'), parts along dimension 0, may hold values from 0 to 3, never falling along the last dimension, each value on 1 to 192 neighbouring positions
- residue_mask: int32 [768], P('grp'), parts along dimension 0, may hold values from 0 to 1, as said below
- chain_vec: float32 [128], replicated, may hold values from -4 to 4
- tri_in: bfloat16 [128, 512], replicated, may hold values from -0.5 to 0.5
- tri_gate: bfloat16 [128, 128], replicated, may hold values from -0.5 to 0.5
- tri_out: bfloat16 [128, 128], replicated, may hold values from -0.5 to 0.5
- att_query: bfloat16 [128, 256], replicated, may hold values from -0.5 to 0.5
- att_kv: bfloat16 [128, 256], replicated, may hold values from -0.5 to 0.5
- att_bias: bfloat16 [128, 4], replicated, may hold values from -0.5 to 0.5
- att_out: bfloat16 [128, 128], replicated, may hold values from -0.5 to 0.5
Outputs:
- updated: bfloat16 [768, 384, 128], P(('grp', 'row'), ('col', 'sub')), parts along dimension 0
The draws below stay inside these ranges and needn't reach their ends.
There are 2 independent parts, one for each index of `grp`. The reference program is written for one: setup_inputs(seed, part) draws one part's arguments, and reference() takes and returns one part's arrays. A program takes and returns all parts, laid end to end along the dimension named above; an argument that names none is the same for every part. Nothing has to cross between parts.
Inputs may be any that keep to these rules, and one draw needn't show every extreme that they name: `chain_ids`: chains are runs of consecutive residues. `residue_mask`: 1 on residues 0 to L - 1 and 0 after them, with L between 192 and 384.
All inputs are finite; a program needn't handle non-finite values.
Results may differ from the reference program's by a relative error of at most 0.009.
Values may be sent and summed in bfloat16 or wider, within the bound.
No kernel may reach another device: no remote copies, remote signals or barrier semaphores. Data moves between devices by JAX's collectives and lax.ppermute only.
A program may use at most 64 MiB of HBM per device.

```python
import math
import jax
import jax.numpy as jnp
import numpy as np
from jax import lax

CHANNELS = 128
HEADS = 4
HEAD_DIM = 32
RESIDUES = 384


def draw_residue_mask(key, part):
    limit = jax.random.randint(jax.random.fold_in(key, 11), (), RESIDUES // 2, RESIDUES + 1)
    return (jnp.arange(RESIDUES) < limit).astype(jnp.int32)


def level_of(stream_key, dims, split, smallest, high):
    gain = 1.0
    for axis_at, blocks in split:
        heights = jax.random.uniform(jax.random.fold_in(jax.random.fold_in(stream_key, 6), axis_at), (blocks,), jnp.float32, smallest / len(split), high / len(split))
        gain = gain * jnp.repeat(jnp.exp(heights), dims[axis_at] // blocks).reshape((-1,) + (1,) * (len(dims) - 1 - axis_at))
    return gain


def length_profile(amount, total, bound, lean):
    portions = [(1 << 20) // math.isqrt(rank ** lean) + 1 for rank in range(2, amount + 1)]
    rest, holding = total - bound - (amount - 1), [1] * (amount - 1)
    while rest > 0:
        movable = [i for i in range(amount - 1) if holding[i] < bound]
        whole, remaining = sum([portions[i] for i in movable]), rest
        for i in movable:
            addition = min(bound - holding[i], max(1, remaining * portions[i] // whole), rest)
            holding[i] = holding[i] + addition
            rest = rest - addition
    return np.array([bound] + holding)


def ragged(stream_key, amount, total, reach, lean):
    if amount == 2:
        one = jax.random.randint(stream_key, (), max(1, total - reach), min(reach, total - 1) + 1)
        return jnp.stack([one, total - one])
    lengths = jnp.asarray(length_profile(amount, total, reach, lean), jnp.int32)
    pairs = (amount - 1) // 2
    source_of, taker = lengths[1:1 + 2 * pairs:2], lengths[2:2 + 2 * pairs:2]
    room = jnp.minimum(source_of - 1, reach - taker)
    moved = jax.random.randint(jax.random.fold_in(stream_key, 1), (pairs,), 0, 1 << 20) % (room + 1)
    lengths = lengths.at[1:1 + 2 * pairs:2].set(source_of - moved).at[2:2 + 2 * pairs:2].set(taker + moved)
    return lengths[jax.random.permutation(jax.random.fold_in(stream_key, 2), amount)]


def noise(key, shape, width, most, cuts=(), dtype=jnp.bfloat16):
    factor_of = level_of(key, shape, cuts, -0.22, 0.18) if cuts else 1.0
    entries = jax.random.normal(key, shape, jnp.float32) * width * factor_of
    return jnp.minimum(jnp.maximum(entries, -most), most).astype(dtype)


def setup_inputs(seed: int = 0, part: int = 0) -> dict:
    key_list = jax.random.split(jax.random.key(seed), 12)
    part_splits = jax.random.split(jax.random.fold_in(key_list[11], part), 12)
    pair = noise(part_splits[0], (RESIDUES, RESIDUES, CHANNELS), 1.0, 6.0, ((0, 16), (1, 16)))
    chain_ids = jnp.searchsorted(jnp.cumsum(ragged(part_splits[1], 4, RESIDUES, RESIDUES // 2, 0)), jnp.arange(RESIDUES), side="right").astype(jnp.int32)
    residue_mask = draw_residue_mask(jax.random.fold_in(jax.random.fold_in(key_list[11], part), 71), part)
    chain_vec = noise(key_list[3], (CHANNELS,), 1.0, 4.0, (), jnp.float32)
    tri_in = noise(key_list[4], (CHANNELS, 4 * CHANNELS), CHANNELS ** -0.5, 0.5)
    tri_gate = noise(key_list[5], (CHANNELS, CHANNELS), CHANNELS ** -0.5, 0.5)
    tri_out = noise(key_list[6], (CHANNELS, CHANNELS), CHANNELS ** -0.5, 0.5)
    att_query = noise(key_list[7], (CHANNELS, 2 * HEADS * HEAD_DIM), CHANNELS ** -0.5, 0.5)
    att_kv = noise(key_list[8], (CHANNELS, 2 * HEADS * HEAD_DIM), CHANNELS ** -0.5, 0.5)
    att_bias = noise(key_list[9], (CHANNELS, HEADS), CHANNELS ** -0.5, 0.5)
    att_out = noise(key_list[10], (HEADS * HEAD_DIM, CHANNELS), (HEADS * HEAD_DIM) ** -0.5, 0.5)
    return {"pair": pair, "chain_ids": chain_ids, "residue_mask": residue_mask, "chain_vec": chain_vec, "tri_in": tri_in, "tri_gate": tri_gate, "tri_out": tri_out, "att_query": att_query, "att_kv": att_kv, "att_bias": att_bias, "att_out": att_out}


EPSILON = 1e-05

def layer_norm(values):
    average = lax.optimization_barrier(jnp.mean(values, axis=-1, keepdims=True))
    centred = values - average
    spread = lax.optimization_barrier(jnp.mean(centred * centred, axis=-1, keepdims=True))
    return centred * lax.rsqrt(spread + EPSILON)

def reference(pair, chain_ids, residue_mask, chain_vec, tri_in, tri_gate, tri_out, att_query, att_kv, att_bias, att_out):
    length = pair.shape[0]
    channels = pair.shape[2]
    heads_width = HEADS * HEAD_DIM
    living = residue_mask.astype(jnp.float32)
    pair_mask = living[:, None] * living[None, :]
    same_chain = (chain_ids[:, None] == chain_ids[None, :]).astype(jnp.float32)
    start_pair = pair.astype(jnp.float32) + same_chain[:, :, None] * chain_vec
    normed = layer_norm(start_pair).astype(jnp.bfloat16)
    flat_rows = normed.reshape(length * length, channels)
    projected = jnp.dot(flat_rows, tri_in, preferred_element_type=jnp.float32).reshape(length, length, 4 * channels)
    left_side = (jax.nn.sigmoid(projected[..., channels:2 * channels]) * projected[..., :channels] * pair_mask[..., None]).astype(jnp.bfloat16)
    right_side = (jax.nn.sigmoid(projected[..., 3 * channels:]) * projected[..., 2 * channels:3 * channels] * pair_mask[..., None]).astype(jnp.bfloat16)
    product = jnp.einsum('ikc,jkc->ijc', left_side.astype(jnp.float32), right_side.astype(jnp.float32)).astype(jnp.bfloat16)
    tri_gating = jax.nn.sigmoid(jnp.dot(flat_rows, tri_gate, preferred_element_type=jnp.float32)).reshape(length, length, channels)
    product_normed = layer_norm(product.astype(jnp.float32)).astype(jnp.bfloat16)
    tri_update = tri_gating * jnp.dot(product_normed.reshape(-1, channels), tri_out, preferred_element_type=jnp.float32).reshape(length, length, channels)
    after_tri = (start_pair + tri_update).astype(jnp.bfloat16)
    second = layer_norm(after_tri.astype(jnp.float32)).astype(jnp.bfloat16)
    flat_second = second.reshape(-1, channels)
    query_gate = jnp.dot(flat_second, att_query, preferred_element_type=jnp.float32).reshape(length, length, 2 * heads_width)
    query = (query_gate[..., :heads_width] * HEAD_DIM ** (-0.5)).astype(jnp.bfloat16).reshape(length, length, HEADS, HEAD_DIM)
    gating = jax.nn.sigmoid(query_gate[..., heads_width:])
    keyval = jnp.dot(flat_second, att_kv, preferred_element_type=jnp.float32).astype(jnp.bfloat16).reshape(length, length, 2 * heads_width)
    key_heads = keyval[..., :heads_width].reshape(length, length, HEADS, HEAD_DIM)
    value_heads = keyval[..., heads_width:].reshape(length, length, HEADS, HEAD_DIM)
    tri_bias = jnp.dot(flat_second, att_bias, preferred_element_type=jnp.float32).astype(jnp.bfloat16).reshape(length, length, HEADS)
    bias_heads = jnp.transpose(tri_bias, (2, 0, 1)).astype(jnp.float32)

    def one_row(operands):
        query_row, key_row, value_row = operands
        scores = jnp.einsum('jhd,khd->hjk', query_row.astype(jnp.float32), key_row.astype(jnp.float32)) + bias_heads
        weights = (jnp.exp(scores) * living[None, None, :]).astype(jnp.bfloat16)
        totals = lax.optimization_barrier(jnp.sum(weights.astype(jnp.float32), axis=2))
        summed = jnp.einsum('hjk,khd->jhd', weights.astype(jnp.float32), value_row.astype(jnp.float32))
        return summed / jnp.transpose(totals)[:, :, None]
    attended = lax.map(one_row, (query, key_heads, value_heads))
    outgoing = (attended.reshape(length, length, heads_width) * gating).astype(jnp.bfloat16)
    result = after_tri.astype(jnp.float32) + jnp.dot(outgoing.reshape(-1, heads_width), att_out, preferred_element_type=jnp.float32).reshape(length, length, channels)
    return result.astype(jnp.bfloat16)
```

```python
import jax
import jax.numpy as jnp
from jax import lax
from jax.experimental import pallas as pl
from jax.experimental.pallas import tpu as pltpu
from jax.sharding import PartitionSpec as P

HEADS = 4
HEAD_DIM = 32
EPSILON = 1e-05
LANES = 128
INTERPRET = False

F32 = jnp.float32
BF16 = jnp.bfloat16


def normalised(values):
    average = jnp.mean(values, axis=-1, keepdims=True)
    centred = values - average
    spread = jnp.mean(centred * centred, axis=-1, keepdims=True)
    return centred * lax.rsqrt(spread + EPSILON)


def sigmoid(values):
    return 1.0 / (1.0 + jnp.exp(-values))


def dot(a, b):
    return jnp.dot(a, b, preferred_element_type=F32)


def dot_t(a, b):
    return lax.dot_general(a, b, (((1,), (1,)), ((), ())), preferred_element_type=F32)


def lane_index(rows):
    return lax.broadcasted_iota(jnp.int32, (rows, LANES), 1)


def roll(values, shift):
    shift = shift % LANES
    return values if shift == 0 else pltpu.roll(values, shift, 1)


def call(kernel, outs, ins, spaces, scratch=(), flops=1 << 22):
    vmem = pl.BlockSpec(memory_space=pltpu.VMEM)
    smem = pl.BlockSpec(memory_space=pltpu.SMEM)
    return pl.pallas_call(
        kernel,
        out_shape=[jax.ShapeDtypeStruct(s, t) for s, t in outs],
        in_specs=[smem if k == "s" else vmem for k in spaces],
        out_specs=[vmem] * len(outs),
        scratch_shapes=list(scratch),
        interpret=INTERPRET,
        cost_estimate=pl.CostEstimate(flops=flops, transcendentals=0, bytes_accessed=1 << 20),
        name=kernel.__name__,
    )(*ins)


def start_block(pair_ref, chain_ref, live_ref, place_ref, vec_ref, rows, cols):
    row_start = place_ref[0]
    col_start = place_ref[1]
    spot = lax.broadcasted_iota(jnp.int32, (cols, LANES), 0)
    col_chain = jnp.zeros((cols, LANES), jnp.int32)
    col_live = jnp.zeros((cols, LANES), jnp.int32)
    for b in range(cols):
        col_chain = jnp.where(spot == b, chain_ref[col_start + b], col_chain)
        col_live = jnp.where(spot == b, live_ref[col_start + b], col_live)
    vec = jnp.broadcast_to(vec_ref[...], (cols, LANES))
    pieces, masks = [], []
    for a in range(rows):
        piece = pair_ref[a * cols : (a + 1) * cols, :].astype(F32)
        same = col_chain == chain_ref[row_start + a]
        pieces.append(piece + jnp.where(same, vec, 0.0))
        masks.append((col_live * live_ref[row_start + a]).astype(F32))
    return jnp.concatenate(pieces, axis=0), jnp.concatenate(masks, axis=0)


def sides_kernel(rows, cols, per_tile, tiles):
    def sides(pair_ref, chain_ref, live_ref, place_ref, vec_ref, tri_in_ref, send_ref):
        start, mask = start_block(pair_ref, chain_ref, live_ref, place_ref, vec_ref, rows, cols)
        normed = normalised(start).astype(BF16).astype(F32) * mask
        weights = tri_in_ref[...].astype(F32).T.astype(BF16)
        width = send_ref.shape[0]
        for t in range(tiles):
            low = t * per_tile * cols
            piece = normed[low : min(low + LANES, rows * cols)]
            if piece.shape[0] < LANES:
                piece = jnp.concatenate([piece, jnp.zeros((LANES - piece.shape[0], LANES), F32)], axis=0)
            projected = dot_t(weights, piece.astype(BF16))
            left = sigmoid(projected[width : 2 * width]) * projected[:width]
            right = sigmoid(projected[3 * width :]) * projected[2 * width : 3 * width]
            send_ref[:, t * LANES : (t + 1) * LANES] = left.astype(BF16)
            send_ref[:, (tiles + t) * LANES : (tiles + t + 1) * LANES] = right.astype(BF16)

    return sides


def gate_kernel(rows, cols):
    def gates(pair_ref, chain_ref, live_ref, place_ref, vec_ref, tri_gate_ref, query_ref, keyval_ref, start_ref, gate_ref, weights_ref):
        start, _ = start_block(pair_ref, chain_ref, live_ref, place_ref, vec_ref, rows, cols)
        start_ref[...] = start
        gate_ref[...] = sigmoid(dot(normalised(start).astype(BF16), tri_gate_ref[...]))
        width = HEADS * HEAD_DIM
        query = query_ref[:, :width].astype(F32)
        keys = keyval_ref[:, :width].astype(F32)
        values = keyval_ref[:, width:].astype(F32)
        lane = lane_index(query.shape[0])
        for h in range(HEADS):
            low = h * HEAD_DIM
            mixed = jnp.where(lane < HEAD_DIM, roll(query, -low), roll(keys, HEAD_DIM - low))
            mixed = jnp.where(lane < 2 * HEAD_DIM, mixed, roll(values, 2 * HEAD_DIM - low))
            mixed = jnp.where(lane < 3 * HEAD_DIM, mixed, 0.0)
            weights_ref[:, h * LANES : (h + 1) * LANES] = mixed.astype(BF16)

    return gates


def product_kernel(rows, cols, nrow, ncol, nsub, per_tile, tiles):
    blocks = nsub * ncol
    packed = LANES // 32
    groups = blocks // packed
    thirds = rows // 8
    length = nrow * rows

    def products(place_ref, gathered_ref, send_ref, left_ref, right_ref, pack_ref):
        sub = place_ref[2]
        lane = lane_index(nrow)

        def unpacked(side, g, a):
            low = (side * tiles + a // per_tile) * LANES
            offset = (a % per_tile) * cols
            mixed = jnp.zeros((nrow, LANES), F32)
            for q in range(packed):
                at = (g * packed + q) * nrow
                piece = gathered_ref[at : at + nrow, low : low + LANES].astype(F32)
                inside = (lane >= q * cols) & (lane < (q + 1) * cols)
                mixed = jnp.where(inside, roll(piece, q * cols - offset), mixed)
            return mixed

        for g in range(groups):
            for a in range(rows):
                left_ref[a * nrow : (a + 1) * nrow, g * LANES : (g + 1) * LANES] = unpacked(0, g, a).astype(BF16)
                right_ref[pl.ds(g * length + a, nrow, stride=rows), :] = unpacked(1, g, a)
        left = left_ref[...]
        for half in range(2):
            chosen = []
            for g in range(groups):
                parts = []
                for q in range(ncol // 2):
                    at = ((half * (ncol // 2) + q) * nsub + sub) * rows
                    parts.append(right_ref[pl.ds(pl.multiple_of(g * length + at, 8), rows), :])
                parts.append(jnp.zeros((LANES - rows * (ncol // 2), LANES), F32))
                chosen.append(jnp.concatenate(parts, axis=0))
            chosen = jnp.concatenate(chosen, axis=1).astype(BF16)
            found = dot_t(left, chosen)
            for q in range(ncol // 2):
                for u in range(8):
                    mixed = jnp.zeros((nrow, LANES), F32)
                    for v in range(thirds):
                        a = u * thirds + v
                        piece = found[a * nrow : (a + 1) * nrow]
                        inside = (lane >= v * cols) & (lane < (v + 1) * cols)
                        mixed = jnp.where(inside, roll(piece, v * cols - q * rows), mixed)
                    pack_ref[pl.ds(u, nrow, stride=8), :] = mixed
                at = (half * (ncol // 2) + q) * nrow * 8
                send_ref[at : at + nrow * 8, :] = pack_ref[...].astype(BF16)

    return products


def middle_kernel(rows, cols):
    def middle(back_ref, start_ref, gate_ref, tri_out_ref, weights_ref, query_ref, bias_ref, after_ref, gating_ref, items_ref, biases_ref, wide_ref):
        channels = back_ref.shape[0] // 8
        wide_ref[...] = back_ref[...].astype(F32)
        used = rows // 8 * cols
        parts = []
        for u in range(8):
            parts.append(wide_ref[pl.ds(u, channels, stride=8), :].T[:used])
        product = jnp.concatenate(parts, axis=0)
        product_normed = normalised(product).astype(BF16)
        after = (start_ref[...] + gate_ref[...] * dot(product_normed, tri_out_ref[...])).astype(BF16)
        after_ref[...] = after
        second = normalised(after.astype(F32)).astype(BF16)
        width = HEADS * HEAD_DIM
        biases_ref[...] = lax.dot_general(bias_ref[...], second, (((1,), (1,)), ((), ())), preferred_element_type=F32).astype(BF16)
        lane = lane_index(rows * cols)
        for h in range(HEADS):
            mixed = dot(second, weights_ref[:, h * LANES : (h + 1) * LANES])
            mixed = jnp.where(lane < HEAD_DIM, mixed * HEAD_DIM ** (-0.5), mixed)
            mixed = jnp.where(lane < 3 * HEAD_DIM, mixed, 1.0)
            items_ref[h * rows * cols : (h + 1) * rows * cols, :] = mixed.astype(BF16)
        gating_ref[...] = sigmoid(dot(second, query_ref[:, width:]))

    return middle


def attend_kernel(items, cols, blocks):
    length = blocks * cols

    def attend(whole_ref, bias_ref, live_ref, send_ref, slab_ref):
        bias = bias_ref[...].astype(F32)
        live = live_ref[...]
        lane = lane_index(length)
        slab_ref[...] = jnp.zeros(slab_ref.shape, F32)
        for a in range(items):
            piece = jnp.concatenate([whole_ref[m, a * cols : (a + 1) * cols, :].astype(F32) for m in range(blocks)], axis=0)
            query = piece[:, :HEAD_DIM].astype(BF16)
            keys = piece[:, HEAD_DIM : 2 * HEAD_DIM].astype(BF16)
            weights = (jnp.exp(dot_t(query, keys) + bias) * live).astype(BF16)
            summed = dot(weights, piece.astype(BF16))
            ratio = summed / roll(summed, -HEAD_DIM)
            group = a % 4
            inside = (lane >= group * HEAD_DIM) & (lane < (group + 1) * HEAD_DIM)
            slab_ref[a // 4] = jnp.where(inside, roll(ratio, (group - 2) * HEAD_DIM), slab_ref[a // 4])
        for part in range(slab_ref.shape[0]):
            for m in range(blocks):
                send_ref[m, part * cols : (part + 1) * cols, :] = slab_ref[part, m * cols : (m + 1) * cols, :].astype(BF16)

    return attend


def finish_kernel(rows, cols, items):
    def finish(back_ref, gating_ref, after_ref, att_out_ref, out_ref):
        lane = lane_index(cols)
        pieces = []
        for a in range(rows):
            group, item = a // items, a % items
            mixed = jnp.zeros((cols, LANES), F32)
            for h in range(HEADS):
                part = back_ref[h * (rows // items) + group, (item // 4) * cols : (item // 4 + 1) * cols, :].astype(F32)
                inside = (lane >= h * HEAD_DIM) & (lane < (h + 1) * HEAD_DIM)
                mixed = jnp.where(inside, roll(part, (h - item % 4) * HEAD_DIM), mixed)
            pieces.append(mixed)
        attended = jnp.concatenate(pieces, axis=0)
        outgoing = (attended * gating_ref[...]).astype(BF16)
        out_ref[...] = (after_ref[...].astype(F32) + dot(outgoing, att_out_ref[...])).astype(BF16)

    return finish


def on_device(
    pair, chain_ids, residue_mask, chain_vec, tri_in, tri_gate, tri_out, att_query, att_kv, att_bias, att_out
):
    rows, cols, channels = pair.shape
    nrow, ncol, nsub = lax.axis_size("row"), lax.axis_size("col"), lax.axis_size("sub")
    positions = rows * cols
    length = chain_ids.shape[0]
    blocks = ncol * nsub
    items = HEADS * rows // blocks
    per_tile = LANES // cols
    tiles = -(-rows // per_tile)
    place = jnp.stack([lax.axis_index("row") * rows, lax.axis_index(("col", "sub")) * cols, lax.axis_index("sub")]).astype(jnp.int32)
    flat = pair.reshape(positions, channels)
    vec = chain_vec.reshape(1, channels)
    common = (flat, chain_ids, residue_mask, place, vec)

    (send,) = call(sides_kernel(rows, cols, per_tile, tiles), [((channels, 2 * tiles * LANES), BF16)], common + (tri_in,), "vsssvv")
    moved = lax.all_to_all(send.reshape(channels, 2, tiles * LANES), ("col", "row"), split_axis=0, concat_axis=0, tiled=True)
    start, tri_gating, head_weights = call(
        gate_kernel(rows, cols),
        [((positions, channels), F32), ((positions, channels), F32), ((channels, HEADS * LANES), BF16)],
        common + (tri_gate, att_query, att_kv),
        "vsssvvvv",
    )
    gathered = lax.all_gather(moved.reshape(channels, 2 * tiles * LANES), "sub", axis=0, tiled=True)
    (products,) = call(
        product_kernel(rows, cols, nrow, ncol, nsub, per_tile, tiles),
        [((nrow * ncol * 8, LANES), BF16)],
        (place, gathered),
        "sv",
        scratch=[
            pltpu.VMEM((length, blocks // 4 * LANES), BF16),
            pltpu.VMEM((blocks // 4 * length, LANES), F32),
            pltpu.VMEM((nrow * 8, LANES), F32),
        ],
    )
    returned = lax.all_to_all(products.reshape(nrow * ncol, 8, LANES), ("col", "row"), split_axis=0, concat_axis=0, tiled=True)
    bias_rows = jnp.pad(att_bias.T, ((0, 8 - HEADS), (0, 0)))
    after, gating, sent_items, biases = call(
        middle_kernel(rows, cols),
        [((positions, channels), BF16), ((positions, channels), F32), ((HEADS * positions, LANES), BF16), ((8, positions), BF16)],
        (returned.reshape(channels * 8, LANES), start, tri_gating, tri_out, head_weights, att_query, bias_rows),
        "vvvvvvv",
        scratch=[pltpu.VMEM((channels * 8, LANES), F32)],
    )
    local_bias = biases[:HEADS].reshape(HEADS, rows, cols)
    repeated = jnp.repeat(local_bias, blocks // HEADS, axis=0)
    bias_slab = lax.all_to_all(repeated, ("col", "sub"), split_axis=0, concat_axis=2, tiled=True)
    copies = jnp.broadcast_to(bias_slab, (nrow, rows, length))
    head_table = lax.all_to_all(copies, "row", split_axis=0, concat_axis=0, tiled=True).reshape(length, length)
    whole = lax.all_to_all(
        sent_items.reshape(blocks, items * cols, LANES), ("col", "sub"), split_axis=0, concat_axis=0, tiled=True
    )
    slabs = -(-items // 4)
    (attended,) = call(
        attend_kernel(items, cols, blocks),
        [((blocks, slabs * cols, LANES), BF16)],
        (whole, head_table, residue_mask.astype(F32).reshape(1, length)),
        "vvv",
        scratch=[pltpu.VMEM((slabs, length, LANES), F32)],
    )
    back = lax.all_to_all(attended, ("col", "sub"), split_axis=0, concat_axis=0, tiled=True)
    (result,) = call(
        finish_kernel(rows, cols, items), [((positions, channels), BF16)], (back, gating, after, att_out), "vvvv"
    )
    return result.reshape(rows, cols, channels)


def solution(mesh):
    return jax.shard_map(
        on_device,
        mesh=mesh,
        in_specs=(P(("grp", "row"), ("col", "sub"), None), P("grp"), P("grp")) + (P(),) * 8,
        out_specs=P(("grp", "row"), ("col", "sub"), None),
        check_vma=False,
    )
```

```python
import jax
import jax.numpy as jnp
from jax import lax
from jax.experimental import pallas as pl
from jax.experimental.pallas import tpu as pltpu
from jax.sharding import PartitionSpec as P

HEADS = 4
HEAD_DIM = 32
EPSILON = 1e-05
LANES = 128
INTERPRET = False

F32 = jnp.float32
BF16 = jnp.bfloat16


def normalised(values):
    average = jnp.mean(values, axis=-1, keepdims=True)
    centred = values - average
    spread = jnp.mean(centred * centred, axis=-1, keepdims=True)
    return centred * lax.rsqrt(spread + EPSILON)


def sigmoid(values):
    return 1.0 / (1.0 + jnp.exp(-values))


def dot(a, b):
    return jnp.dot(a, b, preferred_element_type=F32)


def dot_t(a, b):
    return lax.dot_general(a, b, (((1,), (1,)), ((), ())), preferred_element_type=F32)


def lane_index(rows):
    return lax.broadcasted_iota(jnp.int32, (rows, LANES), 1)


def roll(values, shift):
    shift = shift % LANES
    return values if shift == 0 else pltpu.roll(values, shift, 1)


def call(kernel, outs, ins, spaces, scratch=(), flops=1 << 22):
    vmem = pl.BlockSpec(memory_space=pltpu.VMEM)
    smem = pl.BlockSpec(memory_space=pltpu.SMEM)
    return pl.pallas_call(
        kernel,
        out_shape=[jax.ShapeDtypeStruct(s, t) for s, t in outs],
        in_specs=[smem if k == "s" else vmem for k in spaces],
        out_specs=[vmem] * len(outs),
        scratch_shapes=list(scratch),
        interpret=INTERPRET,
        compiler_params=pltpu.CompilerParams(vmem_limit_bytes=16 << 20),
        cost_estimate=pl.CostEstimate(flops=flops, transcendentals=0, bytes_accessed=1 << 20),
        name=kernel.__name__,
    )(*ins)


def start_block(pair_ref, chain_ref, live_ref, place_ref, vec_ref, rows, cols):
    row_start = place_ref[0]
    col_start = place_ref[1]
    spot = lax.broadcasted_iota(jnp.int32, (cols, LANES), 0)
    col_chain = jnp.zeros((cols, LANES), jnp.int32)
    col_live = jnp.zeros((cols, LANES), jnp.int32)
    for b in range(cols):
        col_chain = jnp.where(spot == b, chain_ref[col_start + b], col_chain)
        col_live = jnp.where(spot == b, live_ref[col_start + b], col_live)
    vec = jnp.broadcast_to(vec_ref[...], (cols, LANES))
    pieces, masks = [], []
    for a in range(rows):
        piece = pair_ref[a * cols : (a + 1) * cols, :].astype(F32)
        same = col_chain == chain_ref[row_start + a]
        pieces.append(piece + jnp.where(same, vec, 0.0))
        masks.append((col_live * live_ref[row_start + a]).astype(F32))
    return jnp.concatenate(pieces, axis=0), jnp.concatenate(masks, axis=0)


def sides_kernel(rows, cols, per_tile, tiles):
    def sides(pair_ref, chain_ref, live_ref, place_ref, vec_ref, tri_in_ref, send_ref):
        start, mask = start_block(pair_ref, chain_ref, live_ref, place_ref, vec_ref, rows, cols)
        normed = normalised(start).astype(BF16).astype(F32) * mask
        weights = tri_in_ref[...].astype(F32).T.astype(BF16)
        width = send_ref.shape[0]
        for t in range(tiles):
            low = t * per_tile * cols
            piece = normed[low : min(low + LANES, rows * cols)]
            if piece.shape[0] < LANES:
                piece = jnp.concatenate([piece, jnp.zeros((LANES - piece.shape[0], LANES), F32)], axis=0)
            projected = dot_t(weights, piece.astype(BF16))
            left = sigmoid(projected[width : 2 * width]) * projected[:width]
            right = sigmoid(projected[3 * width :]) * projected[2 * width : 3 * width]
            send_ref[:, t * LANES : (t + 1) * LANES] = left.astype(BF16)
            send_ref[:, (tiles + t) * LANES : (tiles + t + 1) * LANES] = right.astype(BF16)

    return sides


def gate_kernel(rows, cols):
    def gates(pair_ref, chain_ref, live_ref, place_ref, vec_ref, tri_gate_ref, query_ref, keyval_ref, start_ref, gate_ref, weights_ref):
        start, _ = start_block(pair_ref, chain_ref, live_ref, place_ref, vec_ref, rows, cols)
        start_ref[...] = start
        gate_ref[...] = sigmoid(dot(normalised(start).astype(BF16), tri_gate_ref[...]))
        width = HEADS * HEAD_DIM
        query = query_ref[:, :width].astype(F32)
        keys = keyval_ref[:, :width].astype(F32)
        values = keyval_ref[:, width:].astype(F32)
        lane = lane_index(query.shape[0])
        for h in range(HEADS):
            low = h * HEAD_DIM
            mixed = jnp.where(lane < HEAD_DIM, roll(query, -low), roll(keys, HEAD_DIM - low))
            mixed = jnp.where(lane < 2 * HEAD_DIM, mixed, roll(values, 2 * HEAD_DIM - low))
            mixed = jnp.where(lane < 3 * HEAD_DIM, mixed, 0.0)
            weights_ref[:, h * LANES : (h + 1) * LANES] = mixed.astype(BF16)

    return gates


def product_kernel(rows, cols, nrow, ncol, nsub, per_tile, tiles):
    blocks = nsub * ncol
    packed = LANES // 32
    groups = blocks // packed
    per_out = 4
    length = nrow * rows

    def products(place_ref, gathered_ref, send_ref, left_ref, right_ref):
        sub = place_ref[2]
        lane = lane_index(nrow)

        def unpacked(side, g, a):
            low = (side * tiles + a // per_tile) * LANES
            offset = (a % per_tile) * cols
            mixed = jnp.zeros((nrow, LANES), F32)
            for q in range(packed):
                at = (g * packed + q) * nrow
                piece = gathered_ref[at : at + nrow, low : low + LANES].astype(F32)
                inside = (lane >= q * cols) & (lane < (q + 1) * cols)
                mixed = jnp.where(inside, roll(piece, q * cols - offset), mixed)
            return mixed

        for g in range(groups):
            for a in range(rows):
                left_ref[a * nrow : (a + 1) * nrow, g * LANES : (g + 1) * LANES] = unpacked(0, g, a).astype(BF16)
                right_ref[pl.ds(g * length + a, nrow, stride=rows), :] = unpacked(1, g, a)
        left = left_ref[...]
        for half in range(2):
            chosen = []
            for g in range(groups):
                parts = []
                for q in range(ncol // 2):
                    at = ((half * (ncol // 2) + q) * nsub + sub) * rows
                    parts.append(right_ref[pl.ds(pl.multiple_of(g * length + at, 8), rows), :])
                parts.append(jnp.zeros((LANES - rows * (ncol // 2), LANES), F32))
                chosen.append(jnp.concatenate(parts, axis=0))
            chosen = jnp.concatenate(chosen, axis=1).astype(BF16)
            found = dot_t(left, chosen)
            for q in range(ncol // 2):
                at = (half * (ncol // 2) + q) * nrow
                for u in range(rows // per_out):
                    mixed = jnp.zeros((nrow, LANES), F32)
                    for v in range(per_out):
                        a = u * per_out + v
                        piece = found[a * nrow : (a + 1) * nrow]
                        inside = (lane >= v * cols) & (lane < (v + 1) * cols)
                        mixed = jnp.where(inside, roll(piece, v * cols - q * rows), mixed)
                    send_ref[at : at + nrow, u * LANES : (u + 1) * LANES] = mixed.astype(BF16)

    return products


def middle_kernel(rows, cols, items, per_tile, tiles):
    per_out = 4

    def middle(back_ref, start_ref, gate_ref, tri_out_ref, weights_ref, query_ref, bias_ref, after_ref, gating_ref, items_ref, table_ref):
        positions = rows * cols
        parts = []
        for u in range(rows // per_out):
            parts.append(back_ref[:, u * LANES : (u + 1) * LANES].astype(F32).T[: per_out * cols])
        product = jnp.concatenate(parts, axis=0)
        product_normed = normalised(product).astype(BF16)
        after = (start_ref[...] + gate_ref[...] * dot(product_normed, tri_out_ref[...])).astype(BF16)
        after_ref[...] = after
        second_wide = normalised(after.astype(F32))
        second = second_wide.astype(BF16)
        width = HEADS * HEAD_DIM
        spare = 3 * HEAD_DIM
        lane = lane_index(8)
        for t in range(tiles):
            low = t * per_tile * cols
            piece = second_wide[low : min(low + LANES, positions)]
            if piece.shape[0] < LANES:
                piece = jnp.concatenate([piece, jnp.zeros((LANES - piece.shape[0], LANES), F32)], axis=0)
            found = dot_t(bias_ref[...], piece.astype(BF16))
            for a in range(t * per_tile, min((t + 1) * per_tile, rows)):
                moved = roll(found, spare - (a % per_tile) * cols)
                table_ref[pl.ds(a, 8, stride=rows), :] = jnp.where((lane >= spare) & (lane < spare + cols), moved, 0.0)
        lane = lane_index(positions)
        for h in range(HEADS):
            mixed = dot(second, weights_ref[:, h * LANES : (h + 1) * LANES])
            mixed = jnp.where(lane < HEAD_DIM, mixed * HEAD_DIM ** (-0.5), mixed)
            bias = table_ref[h * rows : (h + 1) * rows, :]
            for group in range(rows // items):
                low = group * items * cols
                at = h * positions + low
                items_ref[at : at + items * cols, :] = jnp.concatenate(
                    [mixed[low : low + rows] + bias, mixed[low + rows : low + items * cols]], axis=0
                ).astype(BF16)
        gating_ref[...] = sigmoid(dot(second, query_ref[:, width:]))

    return middle


def table_kernel(rows, cols, blocks, copies):
    def table(whole_ref, send_ref):
        spare = 3 * HEAD_DIM
        lane = lane_index(rows)
        wide = blocks * cols // LANES
        parts = [jnp.zeros((rows, LANES), F32) for _ in range(wide)]
        for m in range(blocks):
            piece = whole_ref[m, :rows, :].astype(F32)
            moved = roll(piece, m * cols - spare)
            for w in range(wide):
                low, high = max(m * cols - w * LANES, 0), min((m + 1) * cols - w * LANES, LANES)
                if low < high:
                    parts[w] = jnp.where((lane >= low) & (lane < high), moved, parts[w])
        whole = jnp.concatenate(parts, axis=1).astype(BF16)
        for r in range(copies):
            send_ref[r] = whole

    return table


def attend_kernel(items, cols, blocks):
    length = blocks * cols

    def attend(whole_ref, bias_ref, live_ref, send_ref, slab_ref):
        bias = bias_ref[...].astype(F32)
        live = live_ref[...]
        lane = lane_index(length)
        slab_ref[...] = jnp.zeros(slab_ref.shape, F32)
        for a in range(items):
            piece = jnp.concatenate([whole_ref[m, a * cols : (a + 1) * cols, :].astype(F32) for m in range(blocks)], axis=0)
            query = piece[:, :HEAD_DIM].astype(BF16)
            keys = piece[:, HEAD_DIM : 2 * HEAD_DIM].astype(BF16)
            weights = (jnp.exp(dot_t(query, keys) + bias) * live).astype(BF16)
            summed = dot(weights, jnp.where(lane < 3 * HEAD_DIM, piece, 1.0).astype(BF16))
            ratio = summed / roll(summed, -HEAD_DIM)
            group = a % 4
            inside = (lane >= group * HEAD_DIM) & (lane < (group + 1) * HEAD_DIM)
            slab_ref[a // 4] = jnp.where(inside, roll(ratio, (group - 2) * HEAD_DIM), slab_ref[a // 4])
        for part in range(slab_ref.shape[0]):
            for m in range(blocks):
                send_ref[m, part * cols : (part + 1) * cols, :] = slab_ref[part, m * cols : (m + 1) * cols, :].astype(BF16)

    return attend


def finish_kernel(rows, cols, items):
    def finish(back_ref, gating_ref, after_ref, att_out_ref, out_ref):
        lane = lane_index(cols)
        pieces = []
        for a in range(rows):
            group, item = a // items, a % items
            mixed = jnp.zeros((cols, LANES), F32)
            for h in range(HEADS):
                part = back_ref[h * (rows // items) + group, (item // 4) * cols : (item // 4 + 1) * cols, :].astype(F32)
                inside = (lane >= h * HEAD_DIM) & (lane < (h + 1) * HEAD_DIM)
                mixed = jnp.where(inside, roll(part, (h - item % 4) * HEAD_DIM), mixed)
            pieces.append(mixed)
        attended = jnp.concatenate(pieces, axis=0)
        outgoing = (attended * gating_ref[...]).astype(BF16)
        out_ref[...] = (after_ref[...].astype(F32) + dot(outgoing, att_out_ref[...])).astype(BF16)

    return finish


def on_device(
    pair, chain_ids, residue_mask, chain_vec, tri_in, tri_gate, tri_out, att_query, att_kv, att_bias, att_out
):
    rows, cols, channels = pair.shape
    nrow, ncol, nsub = lax.axis_size("row"), lax.axis_size("col"), lax.axis_size("sub")
    positions = rows * cols
    length = chain_ids.shape[0]
    blocks = ncol * nsub
    items = HEADS * rows // blocks
    per_tile = LANES // cols
    tiles = -(-rows // per_tile)
    place = jnp.stack([lax.axis_index("row") * rows, lax.axis_index(("col", "sub")) * cols, lax.axis_index("sub")]).astype(jnp.int32)
    flat = pair.reshape(positions, channels)
    vec = chain_vec.reshape(1, channels)
    common = (flat, chain_ids, residue_mask, place, vec)

    (send,) = call(sides_kernel(rows, cols, per_tile, tiles), [((channels, 2 * tiles * LANES), BF16)], common + (tri_in,), "vsssvv")
    moved = lax.all_to_all(send.reshape(channels, 2, tiles * LANES), ("col", "row"), split_axis=0, concat_axis=0, tiled=True)
    start, tri_gating, head_weights = call(
        gate_kernel(rows, cols),
        [((positions, channels), F32), ((positions, channels), F32), ((channels, HEADS * LANES), BF16)],
        common + (tri_gate, att_query, att_kv),
        "vsssvvvv",
    )
    gathered = lax.all_gather(moved.reshape(channels, 2 * tiles * LANES), "sub", axis=0, tiled=True)
    (products,) = call(
        product_kernel(rows, cols, nrow, ncol, nsub, per_tile, tiles),
        [((nrow * ncol, rows // 4 * LANES), BF16)],
        (place, gathered),
        "sv",
        scratch=[
            pltpu.VMEM((length, blocks // 4 * LANES), BF16),
            pltpu.VMEM((blocks // 4 * length, LANES), F32),
        ],
    )
    returned = lax.all_to_all(products.reshape(nrow * ncol, 2, rows // 8 * LANES), ("col", "row"), split_axis=0, concat_axis=0, tiled=True)
    bias_rows = jnp.pad(att_bias.T, ((0, 8 - HEADS), (0, 0)))
    after, gating, sent_items = call(
        middle_kernel(rows, cols, items, per_tile, tiles),
        [((positions, channels), BF16), ((positions, channels), F32), ((HEADS * positions, LANES), BF16)],
        (returned.reshape(channels, rows // 4 * LANES), start, tri_gating, tri_out, head_weights, att_query, bias_rows),
        "vvvvvvv",
        scratch=[pltpu.VMEM((8 * rows, LANES), F32)],
    )
    whole = lax.all_to_all(
        sent_items.reshape(blocks, items * cols, LANES), ("col", "sub"), split_axis=0, concat_axis=0, tiled=True
    )
    (copies,) = call(table_kernel(rows, cols, blocks, nrow), [((nrow, rows, length), BF16)], (whole,), "v")
    head_table = lax.all_to_all(copies, "row", split_axis=0, concat_axis=0, tiled=True).reshape(length, length)
    slabs = -(-items // 4)
    (attended,) = call(
        attend_kernel(items, cols, blocks),
        [((blocks, slabs * cols, LANES), BF16)],
        (whole, head_table, residue_mask.astype(F32).reshape(1, length)),
        "vvv",
        scratch=[pltpu.VMEM((slabs, length, LANES), F32)],
    )
    back = lax.all_to_all(attended, ("col", "sub"), split_axis=0, concat_axis=0, tiled=True)
    (result,) = call(
        finish_kernel(rows, cols, items), [((positions, channels), BF16)], (back, gating, after, att_out), "vvvv"
    )
    return result.reshape(rows, cols, channels)


def solution(mesh):
    return jax.shard_map(
        on_device,
        mesh=mesh,
        in_specs=(P(("grp", "row"), ("col", "sub"), None), P("grp"), P("grp")) + (P(),) * 8,
        out_specs=P(("grp", "row"), ("col", "sub"), None),
        check_vma=False,
    )
```

```python
import jax
import jax.numpy as jnp
from jax import lax
from jax.experimental import pallas as pl
from jax.experimental.pallas import tpu as pltpu
from jax.sharding import PartitionSpec as P

HEADS = 4
HEAD_DIM = 32
EPSILON = 1e-05
LANES = 128
INTERPRET = False

F32 = jnp.float32
BF16 = jnp.bfloat16


def normalised(values):
    average = jnp.mean(values, axis=-1, keepdims=True)
    centred = values - average
    spread = jnp.mean(centred * centred, axis=-1, keepdims=True)
    return centred * lax.rsqrt(spread + EPSILON)


def sigmoid(values):
    return 1.0 / (1.0 + jnp.exp(-values))


def dot(a, b):
    return jnp.dot(a, b, preferred_element_type=F32)


def dot_t(a, b):
    return lax.dot_general(a, b, (((1,), (1,)), ((), ())), preferred_element_type=F32)


def lane_index(rows):
    return lax.broadcasted_iota(jnp.int32, (rows, LANES), 1)


def roll(values, shift):
    shift = shift % LANES
    return values if shift == 0 else pltpu.roll(values, shift, 1)


def call(kernel, outs, ins, spaces, scratch=(), flops=1 << 22):
    vmem = pl.BlockSpec(memory_space=pltpu.VMEM)
    smem = pl.BlockSpec(memory_space=pltpu.SMEM)
    return pl.pallas_call(
        kernel,
        out_shape=[jax.ShapeDtypeStruct(s, t) for s, t in outs],
        in_specs=[smem if k == "s" else vmem for k in spaces],
        out_specs=[vmem] * len(outs),
        scratch_shapes=list(scratch),
        interpret=INTERPRET,
        compiler_params=pltpu.CompilerParams(vmem_limit_bytes=16 << 20),
        cost_estimate=pl.CostEstimate(flops=flops, transcendentals=0, bytes_accessed=1 << 20),
        name=kernel.__name__,
    )(*ins)


def start_block(pair_ref, chain_ref, live_ref, place_ref, vec_ref, rows, cols):
    row_start = place_ref[0]
    col_start = place_ref[1]
    spot = lax.broadcasted_iota(jnp.int32, (cols, LANES), 0)
    col_chain = jnp.zeros((cols, LANES), jnp.int32)
    col_live = jnp.zeros((cols, LANES), jnp.int32)
    for b in range(cols):
        col_chain = jnp.where(spot == b, chain_ref[col_start + b], col_chain)
        col_live = jnp.where(spot == b, live_ref[col_start + b], col_live)
    vec = jnp.broadcast_to(vec_ref[...], (cols, LANES))
    pieces, masks = [], []
    for a in range(rows):
        piece = pair_ref[a * cols : (a + 1) * cols, :].astype(F32)
        same = col_chain == chain_ref[row_start + a]
        pieces.append(piece + jnp.where(same, vec, 0.0))
        masks.append((col_live * live_ref[row_start + a]).astype(F32))
    return jnp.concatenate(pieces, axis=0), jnp.concatenate(masks, axis=0)


def sides_kernel(rows, cols, per_tile, tiles):
    def sides(pair_ref, chain_ref, live_ref, place_ref, vec_ref, tri_in_ref, send_ref):
        start, mask = start_block(pair_ref, chain_ref, live_ref, place_ref, vec_ref, rows, cols)
        normed = normalised(start).astype(BF16).astype(F32) * mask
        weights = tri_in_ref[...].astype(F32).T.astype(BF16)
        width = send_ref.shape[0]
        for t in range(tiles):
            low = t * per_tile * cols
            piece = normed[low : min(low + LANES, rows * cols)]
            if piece.shape[0] < LANES:
                piece = jnp.concatenate([piece, jnp.zeros((LANES - piece.shape[0], LANES), F32)], axis=0)
            projected = dot_t(weights, piece.astype(BF16))
            left = sigmoid(projected[width : 2 * width]) * projected[:width]
            right = sigmoid(projected[3 * width :]) * projected[2 * width : 3 * width]
            send_ref[:, t * LANES : (t + 1) * LANES] = left.astype(BF16)
            send_ref[:, (tiles + t) * LANES : (tiles + t + 1) * LANES] = right.astype(BF16)

    return sides


def gate_kernel(rows, cols):
    def gates(pair_ref, chain_ref, live_ref, place_ref, vec_ref, tri_gate_ref, query_ref, keyval_ref, start_ref, gate_ref, weights_ref):
        start, _ = start_block(pair_ref, chain_ref, live_ref, place_ref, vec_ref, rows, cols)
        start_ref[...] = start
        gate_ref[...] = sigmoid(dot(normalised(start).astype(BF16), tri_gate_ref[...]))
        width = HEADS * HEAD_DIM
        query = query_ref[:, :width].astype(F32)
        keys = keyval_ref[:, :width].astype(F32)
        values = keyval_ref[:, width:].astype(F32)
        lane = lane_index(query.shape[0])
        for h in range(HEADS):
            low = h * HEAD_DIM
            mixed = jnp.where(lane < HEAD_DIM, roll(query, -low), roll(keys, HEAD_DIM - low))
            mixed = jnp.where(lane < 2 * HEAD_DIM, mixed, roll(values, 2 * HEAD_DIM - low))
            mixed = jnp.where(lane < 3 * HEAD_DIM, mixed, 0.0)
            weights_ref[:, h * LANES : (h + 1) * LANES] = mixed.astype(BF16)

    return gates


def product_kernel(rows, cols, nrow, ncol, nsub, per_tile, tiles):
    blocks = nsub * ncol
    packed = LANES // 32
    groups = blocks // packed
    per_out = 4
    length = nrow * rows

    def products(place_ref, gathered_ref, send_ref, left_ref, right_ref):
        sub = place_ref[2]
        lane = lane_index(nrow)

        def unpacked(side, g, a):
            low = (side * tiles + a // per_tile) * LANES
            offset = (a % per_tile) * cols
            mixed = jnp.zeros((nrow, LANES), F32)
            for q in range(packed):
                at = (g * packed + q) * nrow
                piece = gathered_ref[at : at + nrow, low : low + LANES].astype(F32)
                inside = (lane >= q * cols) & (lane < (q + 1) * cols)
                mixed = jnp.where(inside, roll(piece, q * cols - offset), mixed)
            return mixed

        for g in range(groups):
            for a in range(rows):
                left_ref[a * nrow : (a + 1) * nrow, g * LANES : (g + 1) * LANES] = unpacked(0, g, a).astype(BF16)
                right_ref[pl.ds(g * length + a, nrow, stride=rows), :] = unpacked(1, g, a)
        left = left_ref[...]
        for half in range(2):
            chosen = []
            for g in range(groups):
                parts = []
                for q in range(ncol // 2):
                    at = ((half * (ncol // 2) + q) * nsub + sub) * rows
                    parts.append(right_ref[pl.ds(pl.multiple_of(g * length + at, 8), rows), :])
                parts.append(jnp.zeros((LANES - rows * (ncol // 2), LANES), F32))
                chosen.append(jnp.concatenate(parts, axis=0))
            chosen = jnp.concatenate(chosen, axis=1).astype(BF16)
            found = dot_t(left, chosen)
            for q in range(ncol // 2):
                at = (half * (ncol // 2) + q) * nrow
                for u in range(rows // per_out):
                    mixed = jnp.zeros((nrow, LANES), F32)
                    for v in range(per_out):
                        a = u * per_out + v
                        piece = found[a * nrow : (a + 1) * nrow]
                        inside = (lane >= v * cols) & (lane < (v + 1) * cols)
                        mixed = jnp.where(inside, roll(piece, v * cols - q * rows), mixed)
                    send_ref[at : at + nrow, u * LANES : (u + 1) * LANES] = mixed.astype(BF16)

    return products


def after_kernel(rows, cols, copies, per_tile, tiles):
    per_out = 4

    def after(back_ref, start_ref, gate_ref, tri_out_ref, bias_ref, after_ref, second_ref, send_ref, table_ref):
        positions = rows * cols
        parts = []
        for u in range(rows // per_out):
            parts.append(back_ref[:, u * LANES : (u + 1) * LANES].astype(F32).T[: per_out * cols])
        product = jnp.concatenate(parts, axis=0)
        product_normed = normalised(product).astype(BF16)
        after = (start_ref[...] + gate_ref[...] * dot(product_normed, tri_out_ref[...])).astype(BF16)
        after_ref[...] = after
        second = normalised(after.astype(F32))
        second_ref[...] = second.astype(BF16)
        lane = lane_index(8)
        for t in range(tiles):
            low = t * per_tile * cols
            piece = second[low : min(low + LANES, positions)]
            if piece.shape[0] < LANES:
                piece = jnp.concatenate([piece, jnp.zeros((LANES - piece.shape[0], LANES), F32)], axis=0)
            found = dot_t(bias_ref[...], piece.astype(BF16))
            for a in range(t * per_tile, min((t + 1) * per_tile, rows)):
                moved = roll(found, -(a % per_tile) * cols)
                table_ref[pl.ds(a, 8, stride=rows), :] = jnp.where(lane < cols, moved, 0.0)
        mixed = table_ref[:rows, :]
        for h in range(1, HEADS):
            mixed = mixed + roll(table_ref[h * rows : (h + 1) * rows, :], h * HEAD_DIM)
        mixed = mixed.astype(BF16)
        for r in range(copies):
            send_ref[r] = mixed

    return after


def items_kernel(positions):
    def items(second_ref, weights_ref, query_ref, items_ref, gating_ref):
        second = second_ref[...]
        lane = lane_index(positions)
        for h in range(HEADS):
            mixed = dot(second, weights_ref[:, h * LANES : (h + 1) * LANES])
            mixed = jnp.where(lane < HEAD_DIM, mixed * HEAD_DIM ** (-0.5), mixed)
            items_ref[h * positions : (h + 1) * positions, :] = mixed.astype(BF16)
        gating_ref[...] = sigmoid(dot(second, query_ref[:, HEADS * HEAD_DIM :]))

    return items


def pack_kernel(chunk, cols, length, nsub):
    part = length // nsub
    rest = part - chunk
    spare = 3 * HEAD_DIM
    thin = HEAD_DIM - cols

    def pack(items_ref, table_ref, out_ref):
        lane = lane_index(chunk)
        thin_lane = lane_index(rest)
        for h in range(HEADS):
            extras = []
            for s in range(nsub):
                wide = table_ref[s * part : s * part + chunk, :].astype(F32)
                wide = jnp.where((lane >= spare) & (lane < spare + cols), roll(wide, spare - h * HEAD_DIM), 0.0)
                last = table_ref[s * part + chunk : (s + 1) * part, :].astype(F32)
                pieces = []
                for p in range(chunk // rest):
                    moved = roll(last, spare + cols - h * HEAD_DIM - p * thin)
                    pieces.append(jnp.where(thin_lane >= spare + cols, moved, 0.0))
                extras.append(wide + jnp.concatenate(pieces, axis=0))
            for group in range(HEADS):
                at = (h * HEADS + group) * chunk
                out_ref[at : at + chunk, :] = (items_ref[at : at + chunk, :].astype(F32) + extras[group % nsub]).astype(BF16)

    return pack


def table_kernel(chunk, cols, blocks, length, nsub):
    part = length // nsub
    rest = part - chunk
    spare = 3 * HEAD_DIM
    thin = HEAD_DIM - cols
    wide = length // LANES

    def table(whole_ref, out_ref):
        lane = lane_index(chunk)
        thin_lane = lane_index(rest)
        upper = [jnp.zeros((chunk, LANES), F32) for _ in range(wide)]
        lower = [jnp.zeros((rest, LANES), F32) for _ in range(wide)]
        for m in range(blocks):
            piece = whole_ref[m].astype(F32)
            moved = roll(piece, m * cols - spare)
            for w in range(wide):
                low, high = max(m * cols - w * LANES, 0), min((m + 1) * cols - w * LANES, LANES)
                if low < high:
                    upper[w] = jnp.where((lane >= low) & (lane < high), moved, upper[w])
            for p in range(chunk // rest):
                at = m * cols + p * thin
                moved = roll(piece[p * rest : (p + 1) * rest], at - spare - cols)
                w, low = at // LANES, at % LANES
                lower[w] = jnp.where((thin_lane >= low) & (thin_lane < low + thin), moved, lower[w])
        for w in range(wide):
            out_ref[:chunk, w * LANES : (w + 1) * LANES] = upper[w].astype(BF16)
            out_ref[chunk:, w * LANES : (w + 1) * LANES] = lower[w].astype(BF16)

    return table


def attend_kernel(items, cols, blocks):
    length = blocks * cols

    def attend(whole_ref, bias_ref, live_ref, send_ref, slab_ref):
        bias = bias_ref[...].astype(F32)
        live = live_ref[...]
        lane = lane_index(length)
        slab_ref[...] = jnp.zeros(slab_ref.shape, F32)
        for a in range(items):
            piece = jnp.concatenate([whole_ref[m, a * cols : (a + 1) * cols, :].astype(F32) for m in range(blocks)], axis=0)
            query = piece[:, :HEAD_DIM].astype(BF16)
            keys = piece[:, HEAD_DIM : 2 * HEAD_DIM].astype(BF16)
            weights = (jnp.exp(dot_t(query, keys) + bias) * live).astype(BF16)
            summed = dot(weights, jnp.where(lane < 3 * HEAD_DIM, piece, 1.0).astype(BF16))
            ratio = summed / roll(summed, -HEAD_DIM)
            group = a % 4
            inside = (lane >= group * HEAD_DIM) & (lane < (group + 1) * HEAD_DIM)
            slab_ref[a // 4] = jnp.where(inside, roll(ratio, (group - 2) * HEAD_DIM), slab_ref[a // 4])
        for part in range(slab_ref.shape[0]):
            for m in range(blocks):
                send_ref[m, part * cols : (part + 1) * cols, :] = slab_ref[part, m * cols : (m + 1) * cols, :].astype(BF16)

    return attend


def finish_kernel(rows, cols, items):
    def finish(back_ref, gating_ref, after_ref, att_out_ref, out_ref):
        lane = lane_index(cols)
        pieces = []
        for a in range(rows):
            group, item = a // items, a % items
            mixed = jnp.zeros((cols, LANES), F32)
            for h in range(HEADS):
                part = back_ref[h * (rows // items) + group, (item // 4) * cols : (item // 4 + 1) * cols, :].astype(F32)
                inside = (lane >= h * HEAD_DIM) & (lane < (h + 1) * HEAD_DIM)
                mixed = jnp.where(inside, roll(part, (h - item % 4) * HEAD_DIM), mixed)
            pieces.append(mixed)
        attended = jnp.concatenate(pieces, axis=0)
        outgoing = (attended * gating_ref[...]).astype(BF16)
        out_ref[...] = (after_ref[...].astype(F32) + dot(outgoing, att_out_ref[...])).astype(BF16)

    return finish


def on_device(
    pair, chain_ids, residue_mask, chain_vec, tri_in, tri_gate, tri_out, att_query, att_kv, att_bias, att_out
):
    rows, cols, channels = pair.shape
    nrow, ncol, nsub = lax.axis_size("row"), lax.axis_size("col"), lax.axis_size("sub")
    positions = rows * cols
    length = chain_ids.shape[0]
    blocks = ncol * nsub
    items = HEADS * rows // blocks
    per_tile = LANES // cols
    tiles = -(-rows // per_tile)
    place = jnp.stack([lax.axis_index("row") * rows, lax.axis_index(("col", "sub")) * cols, lax.axis_index("sub")]).astype(jnp.int32)
    flat = pair.reshape(positions, channels)
    vec = chain_vec.reshape(1, channels)
    common = (flat, chain_ids, residue_mask, place, vec)

    (send,) = call(sides_kernel(rows, cols, per_tile, tiles), [((channels, 2 * tiles * LANES), BF16)], common + (tri_in,), "vsssvv")
    moved = lax.all_to_all(send.reshape(channels, 2, tiles * LANES), ("col", "row"), split_axis=0, concat_axis=0, tiled=True)
    start, tri_gating, head_weights = call(
        gate_kernel(rows, cols),
        [((positions, channels), F32), ((positions, channels), F32), ((channels, HEADS * LANES), BF16)],
        common + (tri_gate, att_query, att_kv),
        "vsssvvvv",
    )
    live, start = lax.optimization_barrier((residue_mask.astype(F32).reshape(1, length), start))
    gathered = lax.all_gather(moved.reshape(channels, 2 * tiles * LANES), "sub", axis=0, tiled=True)
    (products,) = call(
        product_kernel(rows, cols, nrow, ncol, nsub, per_tile, tiles),
        [((nrow * ncol, rows // 4 * LANES), BF16)],
        (place, gathered),
        "sv",
        scratch=[
            pltpu.VMEM((length, blocks // 4 * LANES), BF16),
            pltpu.VMEM((blocks // 4 * length, LANES), F32),
        ],
    )
    returned = lax.all_to_all(products.reshape(nrow * ncol, 2, rows // 8 * LANES), ("col", "row"), split_axis=0, concat_axis=0, tiled=True)
    bias_rows = jnp.pad(att_bias.T, ((0, 8 - HEADS), (0, 0)))
    after, second, copies = call(
        after_kernel(rows, cols, nrow, per_tile, tiles),
        [((positions, channels), BF16), ((positions, channels), BF16), ((nrow, rows, LANES), BF16)],
        (returned.reshape(channels, rows // 4 * LANES), start, tri_gating, tri_out, bias_rows),
        "vvvvv",
        scratch=[pltpu.VMEM((8 * rows, LANES), F32)],
    )
    columns = lax.all_to_all(copies, "row", split_axis=0, concat_axis=0, tiled=True)
    plain_items, gating = call(
        items_kernel(positions),
        [((HEADS * positions, LANES), BF16), ((positions, channels), F32)],
        (second, head_weights, att_query),
        "vvv",
    )
    chunk = items * cols
    (sent_items,) = call(
        pack_kernel(chunk, cols, length, nsub),
        [((HEADS * positions, LANES), BF16)],
        (plain_items, columns.reshape(length, LANES)),
        "vv",
    )
    whole = lax.all_to_all(sent_items.reshape(blocks, chunk, LANES), ("col", "sub"), split_axis=0, concat_axis=0, tiled=True)
    (table_part,) = call(table_kernel(chunk, cols, blocks, length, nsub), [((length // nsub, length), BF16)], (whole,), "v")
    head_table = lax.all_gather(table_part, "sub", axis=0, tiled=True)
    slabs = -(-items // 4)
    (attended,) = call(
        attend_kernel(items, cols, blocks),
        [((blocks, slabs * cols, LANES), BF16)],
        (whole, head_table, live),
        "vvv",
        scratch=[pltpu.VMEM((slabs, length, LANES), F32)],
    )
    back = lax.all_to_all(attended, ("col", "sub"), split_axis=0, concat_axis=0, tiled=True)
    (result,) = call(
        finish_kernel(rows, cols, items), [((positions, channels), BF16)], (back, gating, after, att_out), "vvvv"
    )
    return result.reshape(rows, cols, channels)


def solution(mesh):
    return jax.shard_map(
        on_device,
        mesh=mesh,
        in_specs=(P(("grp", "row"), ("col", "sub"), None), P("grp"), P("grp")) + (P(),) * 8,
        out_specs=P(("grp", "row"), ("col", "sub"), None),
        check_vma=False,
    )
```

```python
import jax
import jax.numpy as jnp
from jax import lax
from jax.experimental import pallas as pl
from jax.experimental.pallas import tpu as pltpu
from jax.sharding import PartitionSpec as P

HEADS = 4
HEAD_DIM = 32
EPSILON = 1e-05
LANES = 128
INTERPRET = False

F32 = jnp.float32
BF16 = jnp.bfloat16


def normalised(values):
    average = jnp.mean(values, axis=-1, keepdims=True)
    centred = values - average
    spread = jnp.mean(centred * centred, axis=-1, keepdims=True)
    return centred * lax.rsqrt(spread + EPSILON)


def sigmoid(values):
    return 1.0 / (1.0 + jnp.exp(-values))


def dot(a, b):
    return jnp.dot(a, b, preferred_element_type=F32)


def dot_t(a, b):
    return lax.dot_general(a, b, (((1,), (1,)), ((), ())), preferred_element_type=F32)


def lane_index(rows):
    return lax.broadcasted_iota(jnp.int32, (rows, LANES), 1)


def roll(values, shift):
    shift = shift % LANES
    return values if shift == 0 else pltpu.roll(values, shift, 1)


def in_hbm(values):
    return values if INTERPRET else pltpu.with_memory_space_constraint(values, pltpu.HBM)


def call(kernel, outs, ins, spaces, scratch=(), flops=1 << 22):
    vmem = pl.BlockSpec(memory_space=pltpu.VMEM)
    smem = pl.BlockSpec(memory_space=pltpu.SMEM)
    hbm = pl.BlockSpec(memory_space=pltpu.HBM)
    return pl.pallas_call(
        kernel,
        out_shape=[jax.ShapeDtypeStruct(s, t) for s, t in outs],
        in_specs=[{"s": smem, "v": vmem, "h": hbm}[k] for k in spaces],
        out_specs=[vmem] * len(outs),
        scratch_shapes=list(scratch),
        interpret=INTERPRET,
        compiler_params=pltpu.CompilerParams(vmem_limit_bytes=16 << 20),
        cost_estimate=pl.CostEstimate(flops=flops, transcendentals=0, bytes_accessed=1 << 20),
        name=kernel.__name__,
    )(*ins)


def start_block(pair_ref, chain_ref, live_ref, place_ref, vec_ref, rows, cols):
    row_start = place_ref[0]
    col_start = place_ref[1]
    spot = lax.broadcasted_iota(jnp.int32, (cols, LANES), 0)
    col_chain = jnp.zeros((cols, LANES), jnp.int32)
    col_live = jnp.zeros((cols, LANES), jnp.int32)
    for b in range(cols):
        col_chain = jnp.where(spot == b, chain_ref[col_start + b], col_chain)
        col_live = jnp.where(spot == b, live_ref[col_start + b], col_live)
    vec = jnp.broadcast_to(vec_ref[...], (cols, LANES))
    pieces, masks = [], []
    for a in range(rows):
        piece = pair_ref[a * cols : (a + 1) * cols, :].astype(F32)
        same = col_chain == chain_ref[row_start + a]
        pieces.append(piece + jnp.where(same, vec, 0.0))
        masks.append((col_live * live_ref[row_start + a]).astype(F32))
    return jnp.concatenate(pieces, axis=0), jnp.concatenate(masks, axis=0)


def sides_kernel(rows, cols, per_tile, tiles):
    def sides(place_ref, *refs):
        outside, send_ref, inside, sems = refs[:5], refs[5], refs[6:11], refs[11:]
        copies = [pltpu.make_async_copy(a, b, c) for a, b, c in zip(outside, inside, sems)]
        for copy in copies:
            copy.start()
        for copy in copies:
            copy.wait()
        pair_ref, chain_ref, live_ref, vec_ref, tri_in_ref = inside
        start, mask = start_block(pair_ref, chain_ref, live_ref, place_ref, vec_ref, rows, cols)
        normed = normalised(start).astype(BF16).astype(F32) * mask
        weights = tri_in_ref[...].astype(F32).T.astype(BF16)
        width = send_ref.shape[0]
        for t in range(tiles):
            low = t * per_tile * cols
            piece = normed[low : min(low + LANES, rows * cols)]
            if piece.shape[0] < LANES:
                piece = jnp.concatenate([piece, jnp.zeros((LANES - piece.shape[0], LANES), F32)], axis=0)
            projected = dot_t(weights, piece.astype(BF16))
            left = sigmoid(projected[width : 2 * width]) * projected[:width]
            right = sigmoid(projected[3 * width :]) * projected[2 * width : 3 * width]
            send_ref[:, t * LANES : (t + 1) * LANES] = left.astype(BF16)
            send_ref[:, (tiles + t) * LANES : (tiles + t + 1) * LANES] = right.astype(BF16)

    return sides


def gate_kernel(rows, cols):
    def gates(pair_ref, chain_ref, live_ref, place_ref, vec_ref, tri_gate_ref, query_ref, keyval_ref, tri_out_ref, bias_ref, start_ref, gate_ref, weights_ref, out_ref, wide_ref):
        start, _ = start_block(pair_ref, chain_ref, live_ref, place_ref, vec_ref, rows, cols)
        start_ref[...] = start
        gate_ref[...] = sigmoid(dot(normalised(start).astype(BF16), tri_gate_ref[...]))
        width = HEADS * HEAD_DIM
        query = query_ref[:, :width].astype(F32)
        keys = keyval_ref[:, :width].astype(F32)
        values = keyval_ref[:, width:].astype(F32)
        lane = lane_index(query.shape[0])
        for h in range(HEADS):
            low = h * HEAD_DIM
            mixed = jnp.where(lane < HEAD_DIM, roll(query, -low), roll(keys, HEAD_DIM - low))
            mixed = jnp.where(lane < 2 * HEAD_DIM, mixed, roll(values, 2 * HEAD_DIM - low))
            mixed = jnp.where(lane < 3 * HEAD_DIM, mixed, 0.0)
            weights_ref[:, h * LANES : (h + 1) * LANES] = mixed.astype(BF16)
        out_ref[...] = tri_out_ref[...]
        bias = jnp.concatenate([bias_ref[...].astype(F32), jnp.zeros((LANES - 8, LANES), F32)], axis=0).T
        mixed = jnp.zeros(bias.shape, F32)
        for h in range(HEADS):
            inside = (lane >= h * HEAD_DIM) & (lane < h * HEAD_DIM + cols)
            mixed = jnp.where(inside, bias[:, h : h + 1], mixed)
        wide_ref[...] = mixed.astype(BF16)

    return gates


def product_kernel(rows, cols, nrow, ncol, nsub, per_tile, tiles):
    blocks = nsub * ncol
    packed = LANES // 32
    groups = blocks // packed
    per_out = 4
    length = nrow * rows

    def products(place_ref, gathered_ref, send_ref, left_ref, right_ref):
        sub = place_ref[2]
        lane = lane_index(nrow)

        def unpacked(side, g, a):
            low = (side * tiles + a // per_tile) * LANES
            offset = (a % per_tile) * cols
            mixed = jnp.zeros((nrow, LANES), F32)
            for q in range(packed):
                at = (g * packed + q) * nrow
                piece = gathered_ref[at : at + nrow, low : low + LANES].astype(F32)
                inside = (lane >= q * cols) & (lane < (q + 1) * cols)
                mixed = jnp.where(inside, roll(piece, q * cols - offset), mixed)
            return mixed

        for g in range(groups):
            for a in range(rows):
                left_ref[a * nrow : (a + 1) * nrow, g * LANES : (g + 1) * LANES] = unpacked(0, g, a).astype(BF16)
                right_ref[pl.ds(g * length + a, nrow, stride=rows), :] = unpacked(1, g, a)
        left = left_ref[...]
        for half in range(2):
            chosen = []
            for g in range(groups):
                parts = []
                for q in range(ncol // 2):
                    at = ((half * (ncol // 2) + q) * nsub + sub) * rows
                    parts.append(right_ref[pl.ds(pl.multiple_of(g * length + at, 8), rows), :])
                parts.append(jnp.zeros((LANES - rows * (ncol // 2), LANES), F32))
                chosen.append(jnp.concatenate(parts, axis=0))
            chosen = jnp.concatenate(chosen, axis=1).astype(BF16)
            found = dot_t(left, chosen)
            for q in range(ncol // 2):
                at = (half * (ncol // 2) + q) * nrow
                for u in range(rows // per_out):
                    mixed = jnp.zeros((nrow, LANES), F32)
                    for v in range(per_out):
                        a = u * per_out + v
                        piece = found[a * nrow : (a + 1) * nrow]
                        inside = (lane >= v * cols) & (lane < (v + 1) * cols)
                        mixed = jnp.where(inside, roll(piece, v * cols - q * rows), mixed)
                    send_ref[at : at + nrow, u * LANES : (u + 1) * LANES] = mixed.astype(BF16)

    return products


def after_kernel(rows, cols, copies):
    per_out = 4

    def after(back_ref, start_ref, gate_ref, tri_out_ref, bias_ref, after_ref, second_ref, send_ref):
        positions = rows * cols
        parts = []
        for u in range(rows // per_out):
            parts.append(back_ref[:, u * LANES : (u + 1) * LANES].astype(F32).T[: per_out * cols])
        product = jnp.concatenate(parts, axis=0)
        product_normed = normalised(product).astype(BF16)
        after = (start_ref[...] + gate_ref[...] * dot(product_normed, tri_out_ref[...])).astype(BF16)
        after_ref[...] = after
        second = normalised(after.astype(F32)).astype(BF16)
        second_ref[...] = second
        found = dot(second, bias_ref[...])
        own = lax.broadcasted_iota(jnp.int32, (cols, LANES), 0) == lane_index(cols) % HEAD_DIM
        found = [jnp.where(own, found[a * cols : (a + 1) * cols], 0.0) for a in range(rows)]
        found = jnp.concatenate(found, axis=0).astype(BF16)
        at = lax.broadcasted_iota(jnp.int32, (rows, positions), 0) * cols
        spot = lax.broadcasted_iota(jnp.int32, (rows, positions), 1)
        mine = jnp.where((spot >= at) & (spot < at + cols), 1.0, 0.0).astype(BF16)
        mixed = dot(mine, found).astype(BF16)
        for r in range(copies):
            send_ref[r] = mixed

    return after


def items_kernel(positions):
    def items(second_ref, weights_ref, query_ref, items_ref, gating_ref):
        second = second_ref[...]
        lane = lane_index(positions)
        for h in range(HEADS):
            mixed = dot(second, weights_ref[:, h * LANES : (h + 1) * LANES])
            mixed = jnp.where(lane < HEAD_DIM, mixed * HEAD_DIM ** (-0.5), mixed)
            items_ref[h * positions : (h + 1) * positions, :] = mixed.astype(BF16)
        gating_ref[...] = sigmoid(dot(second, query_ref[:, HEADS * HEAD_DIM :]))

    return items


def pack_kernel(chunk, cols, length, nsub):
    part = length // nsub
    rest = part - chunk
    spare = 3 * HEAD_DIM
    thin = HEAD_DIM - cols

    def pack(items_ref, table_ref, out_ref):
        lane = lane_index(chunk)
        thin_lane = lane_index(rest)
        for h in range(HEADS):
            extras = []
            for s in range(nsub):
                wide = table_ref[s * part : s * part + chunk, :].astype(F32)
                wide = jnp.where((lane >= spare) & (lane < spare + cols), roll(wide, spare - h * HEAD_DIM), 0.0)
                last = table_ref[s * part + chunk : (s + 1) * part, :].astype(F32)
                pieces = []
                for p in range(chunk // rest):
                    moved = roll(last, spare + cols - h * HEAD_DIM - p * thin)
                    pieces.append(jnp.where(thin_lane >= spare + cols, moved, 0.0))
                extras.append(wide + jnp.concatenate(pieces, axis=0))
            for group in range(HEADS):
                at = (h * HEADS + group) * chunk
                out_ref[at : at + chunk, :] = (items_ref[at : at + chunk, :].astype(F32) + extras[group % nsub]).astype(BF16)

    return pack


def table_kernel(chunk, cols, blocks, length, nsub):
    part = length // nsub
    rest = part - chunk
    spare = 3 * HEAD_DIM
    thin = HEAD_DIM - cols
    wide = length // LANES

    def table(whole_ref, out_ref):
        lane = lane_index(chunk)
        thin_lane = lane_index(rest)
        upper = [jnp.zeros((chunk, LANES), F32) for _ in range(wide)]
        lower = [jnp.zeros((rest, LANES), F32) for _ in range(wide)]
        for m in range(blocks):
            piece = whole_ref[m].astype(F32)
            moved = roll(piece, m * cols - spare)
            for w in range(wide):
                low, high = max(m * cols - w * LANES, 0), min((m + 1) * cols - w * LANES, LANES)
                if low < high:
                    upper[w] = jnp.where((lane >= low) & (lane < high), moved, upper[w])
            for p in range(chunk // rest):
                at = m * cols + p * thin
                moved = roll(piece[p * rest : (p + 1) * rest], at - spare - cols)
                w, low = at // LANES, at % LANES
                lower[w] = jnp.where((thin_lane >= low) & (thin_lane < low + thin), moved, lower[w])
        for w in range(wide):
            out_ref[:chunk, w * LANES : (w + 1) * LANES] = upper[w].astype(BF16)
            out_ref[chunk:, w * LANES : (w + 1) * LANES] = lower[w].astype(BF16)

    return table


def attend_kernel(items, cols, blocks):
    length = blocks * cols
    full = items // 4 * 4
    whole_rows = 16

    def attend(whole_ref, bias_ref, live_ref, send_ref):
        bias = jnp.where(live_ref[...] > 0.0, bias_ref[...].astype(F32), -jnp.inf)
        lane = lane_index(length)
        slab = jnp.zeros((length, LANES), F32)
        for a in range(items):
            piece = jnp.concatenate([whole_ref[m, a * cols : (a + 1) * cols, :].astype(F32) for m in range(blocks)], axis=0)
            query = piece[:, :HEAD_DIM].astype(BF16)
            keys = piece[:, HEAD_DIM : 2 * HEAD_DIM].astype(BF16)
            weights = jnp.exp(dot_t(query, keys) + bias).astype(BF16)
            summed = dot(weights, jnp.where(lane < 3 * HEAD_DIM, piece, 1.0).astype(BF16))
            ratio = summed / roll(summed, -HEAD_DIM)
            group = a % 4
            inside = (lane >= group * HEAD_DIM) & (lane < (group + 1) * HEAD_DIM)
            slab = jnp.where(inside, roll(ratio, (group - 2) * HEAD_DIM), slab)
            if a == full - 1:
                for m in range(blocks):
                    send_ref[m, :cols, :] = slab[m * cols : (m + 1) * cols].astype(BF16)
                slab = jnp.zeros((length, LANES), F32)
        moved = roll(slab, 2 * HEAD_DIM)
        moved_on = roll(slab, HEAD_DIM)
        lane = lane_index(8)
        third = (lane >= 2 * HEAD_DIM) & (lane < 3 * HEAD_DIM)
        for m in range(blocks):
            low = m * cols
            tail = low + whole_rows
            out = jnp.concatenate(
                [
                    jnp.where(third, moved[tail : tail + 8], slab[low : low + 8]),
                    jnp.where(third, moved_on[tail : tail + 8], slab[low + 8 : tail]),
                ],
                axis=0,
            )
            send_ref[m, cols:, :] = out.astype(BF16)

    return attend


def finish_kernel(rows, cols, items):
    whole_rows = 16

    def finish(back_ref, gating_ref, after_ref, att_out_ref, out_ref):
        lane = lane_index(cols)
        pieces = []
        for a in range(rows):
            group, item = a // items, a % items
            mixed = jnp.zeros((cols, LANES), F32)
            for h in range(HEADS):
                block = h * (rows // items) + group
                if item < 4:
                    part = roll(back_ref[block, :cols, :].astype(F32), (h - item) * HEAD_DIM)
                else:
                    late = back_ref[block, cols:, :].astype(F32)
                    last = late[(item - 4) * 8 : (item - 3) * 8]
                    part = jnp.concatenate(
                        [roll(late, (h - item + 4) * HEAD_DIM), roll(last, (h - 2) * HEAD_DIM)], axis=0
                    )
                inside = (lane >= h * HEAD_DIM) & (lane < (h + 1) * HEAD_DIM)
                mixed = jnp.where(inside, part, mixed)
            pieces.append(mixed)
        attended = jnp.concatenate(pieces, axis=0)
        outgoing = (attended * gating_ref[...]).astype(BF16)
        out_ref[...] = (after_ref[...].astype(F32) + dot(outgoing, att_out_ref[...])).astype(BF16)

    return finish


def on_device(
    pair, chain_ids, residue_mask, chain_vec, tri_in, tri_gate, tri_out, att_query, att_kv, att_bias, att_out
):
    rows, cols, channels = pair.shape
    nrow, ncol, nsub = lax.axis_size("row"), lax.axis_size("col"), lax.axis_size("sub")
    positions = rows * cols
    length = chain_ids.shape[0]
    blocks = ncol * nsub
    items = HEADS * rows // blocks
    per_tile = LANES // cols
    tiles = -(-rows // per_tile)
    place = jnp.stack([lax.axis_index("row") * rows, lax.axis_index(("col", "sub")) * cols, lax.axis_index("sub")]).astype(jnp.int32)
    flat = pair.reshape(positions, channels)
    vec = chain_vec.reshape(1, channels)
    common = (flat, chain_ids, residue_mask, place, vec)

    (send,) = call(
        sides_kernel(rows, cols, per_tile, tiles),
        [((channels, 2 * tiles * LANES), BF16)],
        (place,) + tuple(in_hbm(x) for x in (flat, chain_ids, residue_mask, vec, tri_in)),
        "shhhhh",
        scratch=[
            pltpu.VMEM(flat.shape, flat.dtype),
            pltpu.SMEM(chain_ids.shape, jnp.int32),
            pltpu.SMEM(residue_mask.shape, jnp.int32),
            pltpu.VMEM(vec.shape, F32),
            pltpu.VMEM(tri_in.shape, tri_in.dtype),
        ]
        + [pltpu.SemaphoreType.DMA] * 5,
    )
    moved = lax.all_to_all(send.reshape(channels, 2, tiles * LANES), ("col", "row"), split_axis=0, concat_axis=0, tiled=True)
    bias_rows = jnp.pad(att_bias.T, ((0, 8 - HEADS), (0, 0)))
    start, tri_gating, head_weights, near_out, wide_bias = call(
        gate_kernel(rows, cols),
        [
            ((positions, channels), F32),
            ((positions, channels), F32),
            ((channels, HEADS * LANES), BF16),
            (tri_out.shape, BF16),
            ((channels, LANES), BF16),
        ],
        common + (tri_gate, att_query, att_kv, tri_out, bias_rows),
        "vsssvvvvvv",
    )
    live, start = lax.optimization_barrier((residue_mask.astype(F32).reshape(1, length), start))
    gathered = lax.all_gather(moved.reshape(channels, 2 * tiles * LANES), "sub", axis=0, tiled=True)
    (products,) = call(
        product_kernel(rows, cols, nrow, ncol, nsub, per_tile, tiles),
        [((nrow * ncol, rows // 4 * LANES), BF16)],
        (place, gathered),
        "sv",
        scratch=[
            pltpu.VMEM((length, blocks // 4 * LANES), BF16),
            pltpu.VMEM((blocks // 4 * length, LANES), F32),
        ],
    )
    returned = lax.all_to_all(products.reshape(nrow * ncol, 2, rows // 8 * LANES), ("col", "row"), split_axis=0, concat_axis=0, tiled=True)
    after, second, copies = call(
        after_kernel(rows, cols, nrow),
        [((positions, channels), BF16), ((positions, channels), BF16), ((nrow, rows, LANES), BF16)],
        (returned.reshape(channels, rows // 4 * LANES), start, tri_gating, near_out, wide_bias),
        "vvvvv",
    )
    columns = lax.all_to_all(copies, "row", split_axis=0, concat_axis=0, tiled=True)
    plain_items, gating = call(
        items_kernel(positions),
        [((HEADS * positions, LANES), BF16), ((positions, channels), F32)],
        (second, head_weights, att_query),
        "vvv",
    )
    chunk = items * cols
    (sent_items,) = call(
        pack_kernel(chunk, cols, length, nsub),
        [((HEADS * positions, LANES), BF16)],
        (plain_items, columns.reshape(length, LANES)),
        "vv",
    )
    whole = lax.all_to_all(sent_items.reshape(blocks, chunk, LANES), ("col", "sub"), split_axis=0, concat_axis=0, tiled=True)
    (table_part,) = call(table_kernel(chunk, cols, blocks, length, nsub), [((length // nsub, length), BF16)], (whole,), "v")
    head_table = lax.all_gather(table_part, "sub", axis=0, tiled=True)
    (attended,) = call(
        attend_kernel(items, cols, blocks), [((blocks, cols + 16, LANES), BF16)], (whole, head_table, live), "vvv"
    )
    back = lax.all_to_all(attended, ("col", "sub"), split_axis=0, concat_axis=0, tiled=True)
    (result,) = call(
        finish_kernel(rows, cols, items), [((positions, channels), BF16)], (back, gating, after, att_out), "vvvv"
    )
    return result.reshape(rows, cols, channels)


def solution(mesh):
    return jax.shard_map(
        on_device,
        mesh=mesh,
        in_specs=(P(("grp", "row"), ("col", "sub"), None), P("grp"), P("grp")) + (P(),) * 8,
        out_specs=P(("grp", "row"), ("col", "sub"), None),
        check_vma=False,
    )
```

```python
import jax
import jax.numpy as jnp
from jax import lax
from jax.experimental import pallas as pl
from jax.experimental.pallas import tpu as pltpu
from jax.sharding import PartitionSpec as P

HEADS = 4
HEAD_DIM = 32
EPSILON = 1e-05
LANES = 128
INTERPRET = False

F32 = jnp.float32
BF16 = jnp.bfloat16


def normalised(values):
    average = jnp.mean(values, axis=-1, keepdims=True)
    centred = values - average
    spread = jnp.mean(centred * centred, axis=-1, keepdims=True)
    return centred * lax.rsqrt(spread + EPSILON)


def sigmoid(values):
    return 1.0 / (1.0 + jnp.exp(-values))


def dot(a, b):
    return jnp.dot(a, b, preferred_element_type=F32)


def dot_t(a, b):
    return lax.dot_general(a, b, (((1,), (1,)), ((), ())), preferred_element_type=F32)


def lane_index(rows):
    return lax.broadcasted_iota(jnp.int32, (rows, LANES), 1)


def roll(values, shift):
    shift = shift % LANES
    return values if shift == 0 else pltpu.roll(values, shift, 1)


def in_hbm(values):
    return values if INTERPRET else pltpu.with_memory_space_constraint(values, pltpu.HBM)


def call(kernel, outs, ins, spaces, scratch=(), flops=1 << 22):
    vmem = pl.BlockSpec(memory_space=pltpu.VMEM)
    smem = pl.BlockSpec(memory_space=pltpu.SMEM)
    hbm = pl.BlockSpec(memory_space=pltpu.HBM)
    return pl.pallas_call(
        kernel,
        out_shape=[jax.ShapeDtypeStruct(s, t) for s, t in outs],
        in_specs=[{"s": smem, "v": vmem, "h": hbm}[k] for k in spaces],
        out_specs=[vmem] * len(outs),
        scratch_shapes=list(scratch),
        interpret=INTERPRET,
        compiler_params=pltpu.CompilerParams(vmem_limit_bytes=16 << 20),
        cost_estimate=pl.CostEstimate(flops=flops, transcendentals=0, bytes_accessed=1 << 20),
        name=kernel.__name__,
    )(*ins)


def start_block(pair_ref, chain_ref, live_ref, place_ref, vec_ref, rows, cols):
    row_start = place_ref[0]
    col_start = place_ref[1]
    spot = lax.broadcasted_iota(jnp.int32, (cols, LANES), 0)
    col_chain = jnp.zeros((cols, LANES), jnp.int32)
    col_live = jnp.zeros((cols, LANES), jnp.int32)
    for b in range(cols):
        col_chain = jnp.where(spot == b, chain_ref[col_start + b], col_chain)
        col_live = jnp.where(spot == b, live_ref[col_start + b], col_live)
    vec = jnp.broadcast_to(vec_ref[...], (cols, LANES))
    pieces, masks = [], []
    for a in range(rows):
        piece = pair_ref[a * cols : (a + 1) * cols, :].astype(F32)
        same = col_chain == chain_ref[row_start + a]
        pieces.append(piece + jnp.where(same, vec, 0.0))
        masks.append((col_live * live_ref[row_start + a]).astype(F32))
    return jnp.concatenate(pieces, axis=0), jnp.concatenate(masks, axis=0)


def sides_kernel(rows, cols, per_tile, tiles):
    def sides(place_ref, *refs):
        outside, send_ref, inside, sems = refs[:5], refs[5], refs[6:11], refs[11:]
        copies = [pltpu.make_async_copy(a, b, c) for a, b, c in zip(outside, inside, sems)]
        for copy in copies:
            copy.start()
        for copy in copies:
            copy.wait()
        pair_ref, chain_ref, live_ref, vec_ref, tri_in_ref = inside
        start, mask = start_block(pair_ref, chain_ref, live_ref, place_ref, vec_ref, rows, cols)
        normed = normalised(start).astype(BF16).astype(F32) * mask
        weights = tri_in_ref[...].astype(F32).T.astype(BF16)
        width = send_ref.shape[0]
        for t in range(tiles):
            low = t * per_tile * cols
            piece = normed[low : min(low + LANES, rows * cols)]
            if piece.shape[0] < LANES:
                piece = jnp.concatenate([piece, jnp.zeros((LANES - piece.shape[0], LANES), F32)], axis=0)
            projected = dot_t(weights, piece.astype(BF16))
            left = sigmoid(projected[width : 2 * width]) * projected[:width]
            right = sigmoid(projected[3 * width :]) * projected[2 * width : 3 * width]
            send_ref[:, t * LANES : (t + 1) * LANES] = left.astype(BF16)
            send_ref[:, (tiles + t) * LANES : (tiles + t + 1) * LANES] = right.astype(BF16)

    return sides


def gate_kernel(rows, cols):
    def gates(pair_ref, chain_ref, live_ref, place_ref, vec_ref, tri_gate_ref, query_ref, keyval_ref, tri_out_ref, bias_ref, start_ref, gate_ref, weights_ref, out_ref, wide_ref):
        start, _ = start_block(pair_ref, chain_ref, live_ref, place_ref, vec_ref, rows, cols)
        start_ref[...] = start
        gate_ref[...] = sigmoid(dot(normalised(start).astype(BF16), tri_gate_ref[...]))
        width = HEADS * HEAD_DIM
        query = query_ref[:, :width].astype(F32)
        keys = keyval_ref[:, :width].astype(F32)
        values = keyval_ref[:, width:].astype(F32)
        lane = lane_index(query.shape[0])
        for h in range(HEADS):
            low = h * HEAD_DIM
            mixed = jnp.where(lane < HEAD_DIM, roll(query, -low), roll(keys, HEAD_DIM - low))
            mixed = jnp.where(lane < 2 * HEAD_DIM, mixed, roll(values, 2 * HEAD_DIM - low))
            mixed = jnp.where(lane < 3 * HEAD_DIM, mixed, 0.0)
            weights_ref[:, h * LANES : (h + 1) * LANES] = mixed.astype(BF16)
        out_ref[...] = tri_out_ref[...]
        bias = jnp.concatenate([bias_ref[...].astype(F32), jnp.zeros((LANES - 8, LANES), F32)], axis=0).T
        mixed = jnp.zeros(bias.shape, F32)
        for h in range(HEADS):
            inside = (lane >= h * HEAD_DIM) & (lane < h * HEAD_DIM + cols)
            mixed = jnp.where(inside, bias[:, h : h + 1], mixed)
        wide_ref[...] = mixed.astype(BF16)

    return gates


def product_kernel(rows, cols, nrow, ncol, nsub, per_tile, tiles):
    blocks = nsub * ncol
    packed = LANES // 32
    groups = blocks // packed
    per_out = 4
    length = nrow * rows

    def products(place_ref, gathered_ref, send_ref, left_ref, right_ref):
        sub = place_ref[2]
        lane = lane_index(nrow)

        def unpacked(side, g, a):
            low = (side * tiles + a // per_tile) * LANES
            offset = (a % per_tile) * cols
            mixed = jnp.zeros((nrow, LANES), F32)
            for q in range(packed):
                at = (g * packed + q) * nrow
                piece = gathered_ref[at : at + nrow, low : low + LANES].astype(F32)
                inside = (lane >= q * cols) & (lane < (q + 1) * cols)
                mixed = jnp.where(inside, roll(piece, q * cols - offset), mixed)
            return mixed

        for g in range(groups):
            for a in range(rows):
                left_ref[a * nrow : (a + 1) * nrow, g * LANES : (g + 1) * LANES] = unpacked(0, g, a).astype(BF16)
                right_ref[pl.ds(g * length + a, nrow, stride=rows), :] = unpacked(1, g, a)
        left = left_ref[...]
        for half in range(2):
            chosen = []
            for g in range(groups):
                parts = []
                for q in range(ncol // 2):
                    at = (((half * (ncol // 2) + q) * nsub + sub) * (nrow // 2 - 1) % nrow) * rows
                    parts.append(right_ref[pl.ds(pl.multiple_of(g * length + at, 8), rows), :])
                parts.append(jnp.zeros((LANES - rows * (ncol // 2), LANES), F32))
                chosen.append(jnp.concatenate(parts, axis=0))
            chosen = jnp.concatenate(chosen, axis=1).astype(BF16)
            found = dot_t(left, chosen)
            for q in range(ncol // 2):
                at = (half * (ncol // 2) + q) * nrow
                for u in range(rows // per_out):
                    mixed = jnp.zeros((nrow, LANES), F32)
                    for v in range(per_out):
                        a = u * per_out + v
                        piece = found[a * nrow : (a + 1) * nrow]
                        inside = (lane >= v * cols) & (lane < (v + 1) * cols)
                        mixed = jnp.where(inside, roll(piece, v * cols - q * rows), mixed)
                    send_ref[at : at + nrow, u * LANES : (u + 1) * LANES] = mixed.astype(BF16)

    return products


def after_kernel(rows, cols, copies):
    per_out = 4

    def after(back_ref, start_ref, gate_ref, tri_out_ref, bias_ref, after_ref, second_ref, send_ref):
        positions = rows * cols
        parts = []
        for u in range(rows // per_out):
            parts.append(back_ref[:, u * LANES : (u + 1) * LANES].astype(F32).T[: per_out * cols])
        product = jnp.concatenate(parts, axis=0)
        product_normed = normalised(product).astype(BF16)
        after = (start_ref[...] + gate_ref[...] * dot(product_normed, tri_out_ref[...])).astype(BF16)
        after_ref[...] = after
        second = normalised(after.astype(F32)).astype(BF16)
        second_ref[...] = second
        found = dot(second, bias_ref[...])
        own = lax.broadcasted_iota(jnp.int32, (cols, LANES), 0) == lane_index(cols) % HEAD_DIM
        found = [jnp.where(own, found[a * cols : (a + 1) * cols], 0.0) for a in range(rows)]
        found = jnp.concatenate(found, axis=0).astype(BF16)
        at = lax.broadcasted_iota(jnp.int32, (rows, positions), 0) * cols
        spot = lax.broadcasted_iota(jnp.int32, (rows, positions), 1)
        mine = jnp.where((spot >= at) & (spot < at + cols), 1.0, 0.0).astype(BF16)
        mixed = dot(mine, found).astype(BF16)
        for r in range(copies):
            send_ref[r] = mixed

    return after


def items_kernel(positions):
    def items(second_ref, weights_ref, query_ref, items_ref, gating_ref):
        second = second_ref[...]
        lane = lane_index(positions)
        for h in range(HEADS):
            mixed = dot(second, weights_ref[:, h * LANES : (h + 1) * LANES])
            mixed = jnp.where(lane < HEAD_DIM, mixed * HEAD_DIM ** (-0.5), mixed)
            items_ref[h * positions : (h + 1) * positions, :] = mixed.astype(BF16)
        gating_ref[...] = sigmoid(dot(second, query_ref[:, HEADS * HEAD_DIM :]))

    return items


def pack_kernel(chunk, cols, length, nsub):
    part = length // nsub
    rest = part - chunk
    spare = 3 * HEAD_DIM
    thin = HEAD_DIM - cols

    def pack(items_ref, table_ref, out_ref):
        lane = lane_index(chunk)
        thin_lane = lane_index(rest)
        for h in range(HEADS):
            extras = []
            for s in range(nsub):
                wide = table_ref[s * part : s * part + chunk, :].astype(F32)
                wide = jnp.where((lane >= spare) & (lane < spare + cols), roll(wide, spare - h * HEAD_DIM), 0.0)
                last = table_ref[s * part + chunk : (s + 1) * part, :].astype(F32)
                pieces = []
                for p in range(chunk // rest):
                    moved = roll(last, spare + cols - h * HEAD_DIM - p * thin)
                    pieces.append(jnp.where(thin_lane >= spare + cols, moved, 0.0))
                extras.append(wide + jnp.concatenate(pieces, axis=0))
            for group in range(HEADS):
                at = (h * HEADS + group) * chunk
                out_ref[at : at + chunk, :] = (items_ref[at : at + chunk, :].astype(F32) + extras[group % nsub]).astype(BF16)

    return pack


def table_kernel(chunk, cols, blocks, length, nsub):
    part = length // nsub
    rest = part - chunk
    spare = 3 * HEAD_DIM
    thin = HEAD_DIM - cols
    wide = length // LANES

    def table(whole_ref, out_ref):
        lane = lane_index(chunk)
        thin_lane = lane_index(rest)
        upper = [jnp.zeros((chunk, LANES), F32) for _ in range(wide)]
        lower = [jnp.zeros((rest, LANES), F32) for _ in range(wide)]
        for m in range(blocks):
            piece = whole_ref[m].astype(F32)
            moved = roll(piece, m * cols - spare)
            for w in range(wide):
                low, high = max(m * cols - w * LANES, 0), min((m + 1) * cols - w * LANES, LANES)
                if low < high:
                    upper[w] = jnp.where((lane >= low) & (lane < high), moved, upper[w])
            for p in range(chunk // rest):
                at = m * cols + p * thin
                moved = roll(piece[p * rest : (p + 1) * rest], at - spare - cols)
                w, low = at // LANES, at % LANES
                lower[w] = jnp.where((thin_lane >= low) & (thin_lane < low + thin), moved, lower[w])
        for w in range(wide):
            out_ref[:chunk, w * LANES : (w + 1) * LANES] = upper[w].astype(BF16)
            out_ref[chunk:, w * LANES : (w + 1) * LANES] = lower[w].astype(BF16)

    return table


def attend_kernel(items, cols, blocks):
    length = blocks * cols
    full = items // 4 * 4
    whole_rows = 16

    def attend(whole_ref, bias_ref, live_ref, send_ref):
        bias = jnp.where(live_ref[...] > 0.0, bias_ref[...].astype(F32), -jnp.inf)
        lane = lane_index(length)
        slab = jnp.zeros((length, LANES), F32)
        for a in range(items):
            piece = jnp.concatenate([whole_ref[m, a * cols : (a + 1) * cols, :].astype(F32) for m in range(blocks)], axis=0)
            query = piece[:, :HEAD_DIM].astype(BF16)
            keys = piece[:, HEAD_DIM : 2 * HEAD_DIM].astype(BF16)
            weights = jnp.exp(dot_t(query, keys) + bias).astype(BF16)
            summed = dot(weights, jnp.where(lane < 3 * HEAD_DIM, piece, 1.0).astype(BF16))
            ratio = summed / roll(summed, -HEAD_DIM)
            group = a % 4
            inside = (lane >= group * HEAD_DIM) & (lane < (group + 1) * HEAD_DIM)
            slab = jnp.where(inside, roll(ratio, (group - 2) * HEAD_DIM), slab)
            if a == full - 1:
                for m in range(blocks):
                    send_ref[m, :cols, :] = slab[m * cols : (m + 1) * cols].astype(BF16)
                slab = jnp.zeros((length, LANES), F32)
        moved = roll(slab, 2 * HEAD_DIM)
        moved_on = roll(slab, HEAD_DIM)
        lane = lane_index(8)
        third = (lane >= 2 * HEAD_DIM) & (lane < 3 * HEAD_DIM)
        for m in range(blocks):
            low = m * cols
            tail = low + whole_rows
            out = jnp.concatenate(
                [
                    jnp.where(third, moved[tail : tail + 8], slab[low : low + 8]),
                    jnp.where(third, moved_on[tail : tail + 8], slab[low + 8 : tail]),
                ],
                axis=0,
            )
            send_ref[m, cols:, :] = out.astype(BF16)

    return attend


def finish_kernel(rows, cols, items):
    whole_rows = 16

    def finish(back_ref, gating_ref, after_ref, att_out_ref, out_ref):
        lane = lane_index(cols)
        pieces = []
        for a in range(rows):
            group, item = a // items, a % items
            mixed = jnp.zeros((cols, LANES), F32)
            for h in range(HEADS):
                block = h * (rows // items) + group
                if item < 4:
                    part = roll(back_ref[block, :cols, :].astype(F32), (h - item) * HEAD_DIM)
                else:
                    late = back_ref[block, cols:, :].astype(F32)
                    last = late[(item - 4) * 8 : (item - 3) * 8]
                    part = jnp.concatenate(
                        [roll(late, (h - item + 4) * HEAD_DIM), roll(last, (h - 2) * HEAD_DIM)], axis=0
                    )
                inside = (lane >= h * HEAD_DIM) & (lane < (h + 1) * HEAD_DIM)
                mixed = jnp.where(inside, part, mixed)
            pieces.append(mixed)
        attended = jnp.concatenate(pieces, axis=0)
        outgoing = (attended * gating_ref[...]).astype(BF16)
        out_ref[...] = (after_ref[...].astype(F32) + dot(outgoing, att_out_ref[...])).astype(BF16)

    return finish


def member_order(nrow, ncol):
    step = nrow // 2 - 1
    return [[c * nrow + step * p % nrow for c in range(ncol) for p in range(nrow)]]


def on_device(
    pair, chain_ids, residue_mask, chain_vec, tri_in, tri_gate, tri_out, att_query, att_kv, att_bias, att_out
):
    rows, cols, channels = pair.shape
    nrow, ncol, nsub = lax.axis_size("row"), lax.axis_size("col"), lax.axis_size("sub")
    order = member_order(nrow, ncol)
    positions = rows * cols
    length = chain_ids.shape[0]
    blocks = ncol * nsub
    items = HEADS * rows // blocks
    per_tile = LANES // cols
    tiles = -(-rows // per_tile)
    place = jnp.stack([lax.axis_index("row") * rows, lax.axis_index(("col", "sub")) * cols, lax.axis_index("sub")]).astype(jnp.int32)
    flat = pair.reshape(positions, channels)
    vec = chain_vec.reshape(1, channels)
    common = (flat, chain_ids, residue_mask, place, vec)

    (send,) = call(
        sides_kernel(rows, cols, per_tile, tiles),
        [((channels, 2 * tiles * LANES), BF16)],
        (place,) + tuple(in_hbm(x) for x in (flat, chain_ids, residue_mask, vec, tri_in)),
        "shhhhh",
        scratch=[
            pltpu.VMEM(flat.shape, flat.dtype),
            pltpu.SMEM(chain_ids.shape, jnp.int32),
            pltpu.SMEM(residue_mask.shape, jnp.int32),
            pltpu.VMEM(vec.shape, F32),
            pltpu.VMEM(tri_in.shape, tri_in.dtype),
        ]
        + [pltpu.SemaphoreType.DMA] * 5,
    )
    moved = lax.all_to_all(send.reshape(channels, 2, tiles * LANES), ("col", "row"), split_axis=0, concat_axis=0, tiled=True, axis_index_groups=order)
    bias_rows = jnp.pad(att_bias.T, ((0, 8 - HEADS), (0, 0)))
    start, tri_gating, head_weights, near_out, wide_bias = call(
        gate_kernel(rows, cols),
        [
            ((positions, channels), F32),
            ((positions, channels), F32),
            ((channels, HEADS * LANES), BF16),
            (tri_out.shape, BF16),
            ((channels, LANES), BF16),
        ],
        common + (tri_gate, att_query, att_kv, tri_out, bias_rows),
        "vsssvvvvvv",
    )
    live, start = lax.optimization_barrier((residue_mask.astype(F32).reshape(1, length), start))
    gathered = lax.all_gather(moved.reshape(channels, 2 * tiles * LANES), "sub", axis=0, tiled=True)
    (products,) = call(
        product_kernel(rows, cols, nrow, ncol, nsub, per_tile, tiles),
        [((nrow * ncol, rows // 4 * LANES), BF16)],
        (place, gathered),
        "sv",
        scratch=[
            pltpu.VMEM((length, blocks // 4 * LANES), BF16),
            pltpu.VMEM((blocks // 4 * length, LANES), F32),
        ],
    )
    returned = lax.all_to_all(products.reshape(nrow * ncol, 2, rows // 8 * LANES), ("col", "row"), split_axis=0, concat_axis=0, tiled=True, axis_index_groups=order)
    after, second, copies = call(
        after_kernel(rows, cols, nrow),
        [((positions, channels), BF16), ((positions, channels), BF16), ((nrow, rows, LANES), BF16)],
        (returned.reshape(channels, rows // 4 * LANES), start, tri_gating, near_out, wide_bias),
        "vvvvv",
    )
    columns = lax.all_to_all(copies, "row", split_axis=0, concat_axis=0, tiled=True)
    plain_items, gating = call(
        items_kernel(positions),
        [((HEADS * positions, LANES), BF16), ((positions, channels), F32)],
        (second, head_weights, att_query),
        "vvv",
    )
    chunk = items * cols
    (sent_items,) = call(
        pack_kernel(chunk, cols, length, nsub),
        [((HEADS * positions, LANES), BF16)],
        (plain_items, columns.reshape(length, LANES)),
        "vv",
    )
    whole = lax.all_to_all(sent_items.reshape(blocks, chunk, LANES), ("col", "sub"), split_axis=0, concat_axis=0, tiled=True)
    (table_part,) = call(table_kernel(chunk, cols, blocks, length, nsub), [((length // nsub, length), BF16)], (whole,), "v")
    head_table = lax.all_gather(table_part, "sub", axis=0, tiled=True)
    (attended,) = call(
        attend_kernel(items, cols, blocks), [((blocks, cols + 16, LANES), BF16)], (whole, head_table, live), "vvv"
    )
    back = lax.all_to_all(attended, ("col", "sub"), split_axis=0, concat_axis=0, tiled=True)
    (result,) = call(
        finish_kernel(rows, cols, items), [((positions, channels), BF16)], (back, gating, after, att_out), "vvvv"
    )
    return result.reshape(rows, cols, channels)


def solution(mesh):
    return jax.shard_map(
        on_device,
        mesh=mesh,
        in_specs=(P(("grp", "row"), ("col", "sub"), None), P("grp"), P("grp")) + (P(),) * 8,
        out_specs=P(("grp", "row"), ("col", "sub"), None),
        check_vma=False,
    )
```

```python
import jax
import jax.numpy as jnp
from jax import lax
from jax.experimental import pallas as pl
from jax.experimental.pallas import tpu as pltpu
from jax.sharding import PartitionSpec as P

HEADS = 4
HEAD_DIM = 32
EPSILON = 1e-05
LANES = 128
INTERPRET = False

F32 = jnp.float32
BF16 = jnp.bfloat16


def normalised(values):
    average = jnp.mean(values, axis=-1, keepdims=True)
    centred = values - average
    spread = jnp.mean(centred * centred, axis=-1, keepdims=True)
    return centred * lax.rsqrt(spread + EPSILON)


def sigmoid(values):
    return 1.0 / (1.0 + jnp.exp(-values))


def dot(a, b):
    return jnp.dot(a, b, preferred_element_type=F32)


def dot_t(a, b):
    return lax.dot_general(a, b, (((1,), (1,)), ((), ())), preferred_element_type=F32)


def lane_index(rows):
    return lax.broadcasted_iota(jnp.int32, (rows, LANES), 1)


def roll(values, shift):
    shift = shift % LANES
    return values if shift == 0 else pltpu.roll(values, shift, 1)


def in_hbm(values):
    return values if INTERPRET else pltpu.with_memory_space_constraint(values, pltpu.HBM)


def call(kernel, outs, ins, spaces, scratch=(), flops=1 << 22):
    vmem = pl.BlockSpec(memory_space=pltpu.VMEM)
    smem = pl.BlockSpec(memory_space=pltpu.SMEM)
    hbm = pl.BlockSpec(memory_space=pltpu.HBM)
    return pl.pallas_call(
        kernel,
        out_shape=[jax.ShapeDtypeStruct(s, t) for s, t in outs],
        in_specs=[{"s": smem, "v": vmem, "h": hbm}[k] for k in spaces],
        out_specs=[vmem] * len(outs),
        scratch_shapes=list(scratch),
        interpret=INTERPRET,
        compiler_params=pltpu.CompilerParams(vmem_limit_bytes=16 << 20),
        cost_estimate=pl.CostEstimate(flops=flops, transcendentals=0, bytes_accessed=1 << 20),
        name=kernel.__name__,
    )(*ins)


def start_block(pair_ref, chain_ref, live_ref, place_ref, vec_ref, rows, cols):
    row_start = place_ref[0]
    col_start = place_ref[1]
    spot = lax.broadcasted_iota(jnp.int32, (cols, LANES), 0)
    col_chain = jnp.zeros((cols, LANES), jnp.int32)
    col_live = jnp.zeros((cols, LANES), jnp.int32)
    for b in range(cols):
        col_chain = jnp.where(spot == b, chain_ref[col_start + b], col_chain)
        col_live = jnp.where(spot == b, live_ref[col_start + b], col_live)
    vec = jnp.broadcast_to(vec_ref[...], (cols, LANES))
    pieces, masks = [], []
    for a in range(rows):
        piece = pair_ref[a * cols : (a + 1) * cols, :].astype(F32)
        same = col_chain == chain_ref[row_start + a]
        pieces.append(piece + jnp.where(same, vec, 0.0))
        masks.append((col_live * live_ref[row_start + a]).astype(F32))
    return jnp.concatenate(pieces, axis=0), jnp.concatenate(masks, axis=0)


def sides_kernel(rows, cols, per_tile, tiles):
    def sides(place_ref, *refs):
        outside, send_ref, inside, sems = refs[:5], refs[5], refs[6:11], refs[11:]
        copies = [pltpu.make_async_copy(a, b, c) for a, b, c in zip(outside, inside, sems)]
        for copy in copies:
            copy.start()
        for copy in copies[:4]:
            copy.wait()
        pair_ref, chain_ref, live_ref, vec_ref, tri_in_ref = inside
        start, mask = start_block(pair_ref, chain_ref, live_ref, place_ref, vec_ref, rows, cols)
        normed = normalised(start).astype(BF16).astype(F32) * mask
        copies[4].wait()
        weights = tri_in_ref[...].astype(F32).T.astype(BF16)
        width = send_ref.shape[0]
        for t in range(tiles):
            low = t * per_tile * cols
            piece = normed[low : min(low + LANES, rows * cols)]
            if piece.shape[0] < LANES:
                piece = jnp.concatenate([piece, jnp.zeros((LANES - piece.shape[0], LANES), F32)], axis=0)
            projected = dot_t(weights, piece.astype(BF16))
            left = sigmoid(projected[width : 2 * width]) * projected[:width]
            right = sigmoid(projected[3 * width :]) * projected[2 * width : 3 * width]
            send_ref[:, t * LANES : (t + 1) * LANES] = left.astype(BF16)
            send_ref[:, (tiles + t) * LANES : (tiles + t + 1) * LANES] = right.astype(BF16)

    return sides


def gate_kernel(rows, cols):
    def gates(pair_ref, chain_ref, live_ref, place_ref, vec_ref, tri_gate_ref, query_ref, keyval_ref, tri_out_ref, bias_ref, start_ref, gate_ref, weights_ref, out_ref, wide_ref):
        start, _ = start_block(pair_ref, chain_ref, live_ref, place_ref, vec_ref, rows, cols)
        start_ref[...] = start
        gate_ref[...] = sigmoid(dot(normalised(start).astype(BF16), tri_gate_ref[...]))
        width = HEADS * HEAD_DIM
        query = query_ref[:, :width].astype(F32)
        keys = keyval_ref[:, :width].astype(F32)
        values = keyval_ref[:, width:].astype(F32)
        lane = lane_index(query.shape[0])
        for h in range(HEADS):
            low = h * HEAD_DIM
            mixed = jnp.where(lane < HEAD_DIM, roll(query, -low), roll(keys, HEAD_DIM - low))
            mixed = jnp.where(lane < 2 * HEAD_DIM, mixed, roll(values, 2 * HEAD_DIM - low))
            mixed = jnp.where(lane < 3 * HEAD_DIM, mixed, 0.0)
            weights_ref[:, h * LANES : (h + 1) * LANES] = mixed.astype(BF16)
        out_ref[...] = tri_out_ref[...]
        bias = jnp.concatenate([bias_ref[...].astype(F32), jnp.zeros((LANES - 8, LANES), F32)], axis=0).T
        mixed = jnp.zeros(bias.shape, F32)
        for h in range(HEADS):
            inside = (lane >= h * HEAD_DIM) & (lane < h * HEAD_DIM + cols)
            mixed = jnp.where(inside, bias[:, h : h + 1], mixed)
        wide_ref[...] = mixed.astype(BF16)

    return gates


def product_kernel(rows, cols, nrow, ncol, nsub, per_tile, tiles):
    blocks = nsub * ncol
    packed = LANES // 32
    groups = blocks // packed
    per_out = 4
    length = nrow * rows

    def products(place_ref, gathered_ref, send_ref, left_ref, right_ref):
        sub = place_ref[2]
        lane = lane_index(nrow)

        def unpacked(side, g, a):
            low = (side * tiles + a // per_tile) * LANES
            offset = (a % per_tile) * cols
            mixed = jnp.zeros((nrow, LANES), F32)
            for q in range(packed):
                at = (g * packed + q) * nrow
                piece = gathered_ref[at : at + nrow, low : low + LANES].astype(F32)
                inside = (lane >= q * cols) & (lane < (q + 1) * cols)
                mixed = jnp.where(inside, roll(piece, q * cols - offset), mixed)
            return mixed

        for g in range(groups):
            for a in range(rows):
                left_ref[a * nrow : (a + 1) * nrow, g * LANES : (g + 1) * LANES] = unpacked(0, g, a).astype(BF16)
                right_ref[pl.ds(g * length + a, nrow, stride=rows), :] = unpacked(1, g, a)
        left = left_ref[...]
        for half in range(2):
            chosen = []
            for g in range(groups):
                parts = []
                for q in range(ncol // 2):
                    at = ((half * (ncol // 2) + q) * nsub + sub) * rows
                    parts.append(right_ref[pl.ds(pl.multiple_of(g * length + at, 8), rows), :])
                parts.append(jnp.zeros((LANES - rows * (ncol // 2), LANES), F32))
                chosen.append(jnp.concatenate(parts, axis=0))
            chosen = jnp.concatenate(chosen, axis=1).astype(BF16)
            found = dot_t(left, chosen)
            for q in range(ncol // 2):
                at = (half * (ncol // 2) + q) * nrow
                for u in range(rows // per_out):
                    mixed = jnp.zeros((nrow, LANES), F32)
                    for v in range(per_out):
                        a = u * per_out + v
                        piece = found[a * nrow : (a + 1) * nrow]
                        inside = (lane >= v * cols) & (lane < (v + 1) * cols)
                        mixed = jnp.where(inside, roll(piece, v * cols - q * rows), mixed)
                    send_ref[at : at + nrow, u * LANES : (u + 1) * LANES] = mixed.astype(BF16)

    return products


def after_kernel(rows, cols, copies):
    per_out = 4

    def after(back_ref, start_ref, gate_ref, tri_out_ref, bias_ref, after_ref, second_ref, send_ref):
        positions = rows * cols
        parts = []
        for u in range(rows // per_out):
            parts.append(back_ref[:, u * LANES : (u + 1) * LANES].astype(F32).T[: per_out * cols])
        product = jnp.concatenate(parts, axis=0)
        product_normed = normalised(product).astype(BF16)
        after = (start_ref[...] + gate_ref[...] * dot(product_normed, tri_out_ref[...])).astype(BF16)
        after_ref[...] = after
        second = normalised(after.astype(F32)).astype(BF16)
        second_ref[...] = second
        found = dot(second, bias_ref[...])
        own = lax.broadcasted_iota(jnp.int32, (cols, LANES), 0) == lane_index(cols) % HEAD_DIM
        found = [jnp.where(own, found[a * cols : (a + 1) * cols], 0.0) for a in range(rows)]
        found = jnp.concatenate(found, axis=0).astype(BF16)
        at = lax.broadcasted_iota(jnp.int32, (rows, positions), 0) * cols
        spot = lax.broadcasted_iota(jnp.int32, (rows, positions), 1)
        mine = jnp.where((spot >= at) & (spot < at + cols), 1.0, 0.0).astype(BF16)
        mixed = dot(mine, found).astype(BF16)
        for r in range(copies):
            send_ref[r] = mixed

    return after


def items_kernel(positions):
    def items(second_ref, weights_ref, query_ref, items_ref, gating_ref):
        second = second_ref[...]
        lane = lane_index(positions)
        for h in range(HEADS):
            mixed = dot(second, weights_ref[:, h * LANES : (h + 1) * LANES])
            mixed = jnp.where(lane < HEAD_DIM, mixed * HEAD_DIM ** (-0.5), mixed)
            items_ref[h * positions : (h + 1) * positions, :] = mixed.astype(BF16)
        gating_ref[...] = sigmoid(dot(second, query_ref[:, HEADS * HEAD_DIM :]))

    return items


def pack_kernel(chunk, cols, length, nsub):
    part = length // nsub
    rest = part - chunk
    spare = 3 * HEAD_DIM
    thin = HEAD_DIM - cols

    def pack(items_ref, table_ref, out_ref):
        lane = lane_index(chunk)
        thin_lane = lane_index(rest)
        for h in range(HEADS):
            extras = []
            for s in range(nsub):
                wide = table_ref[s * part : s * part + chunk, :].astype(F32)
                wide = jnp.where((lane >= spare) & (lane < spare + cols), roll(wide, spare - h * HEAD_DIM), 0.0)
                last = table_ref[s * part + chunk : (s + 1) * part, :].astype(F32)
                pieces = []
                for p in range(chunk // rest):
                    moved = roll(last, spare + cols - h * HEAD_DIM - p * thin)
                    pieces.append(jnp.where(thin_lane >= spare + cols, moved, 0.0))
                extras.append(wide + jnp.concatenate(pieces, axis=0))
            for group in range(HEADS):
                at = (h * HEADS + group) * chunk
                out_ref[at : at + chunk, :] = (items_ref[at : at + chunk, :].astype(F32) + extras[group % nsub]).astype(BF16)

    return pack


def table_kernel(chunk, cols, blocks, length, nsub):
    part = length // nsub
    rest = part - chunk
    spare = 3 * HEAD_DIM
    thin = HEAD_DIM - cols
    wide = length // LANES

    def table(whole_ref, out_ref):
        lane = lane_index(chunk)
        thin_lane = lane_index(rest)
        upper = [jnp.zeros((chunk, LANES), F32) for _ in range(wide)]
        lower = [jnp.zeros((rest, LANES), F32) for _ in range(wide)]
        for m in range(blocks):
            piece = whole_ref[m].astype(F32)
            moved = roll(piece, m * cols - spare)
            for w in range(wide):
                low, high = max(m * cols - w * LANES, 0), min((m + 1) * cols - w * LANES, LANES)
                if low < high:
                    upper[w] = jnp.where((lane >= low) & (lane < high), moved, upper[w])
            for p in range(chunk // rest):
                at = m * cols + p * thin
                moved = roll(piece[p * rest : (p + 1) * rest], at - spare - cols)
                w, low = at // LANES, at % LANES
                lower[w] = jnp.where((thin_lane >= low) & (thin_lane < low + thin), moved, lower[w])
        for w in range(wide):
            out_ref[:chunk, w * LANES : (w + 1) * LANES] = upper[w].astype(BF16)
            out_ref[chunk:, w * LANES : (w + 1) * LANES] = lower[w].astype(BF16)

    return table


def attend_kernel(items, cols, blocks):
    length = blocks * cols
    full = items // 4 * 4
    whole_rows = 16

    def attend(whole_ref, bias_ref, live_ref, send_ref):
        bias = jnp.where(live_ref[...] > 0.0, bias_ref[...].astype(F32), -jnp.inf)
        lane = lane_index(length)
        slab = jnp.zeros((length, LANES), F32)
        for a in range(items):
            piece = jnp.concatenate([whole_ref[m, a * cols : (a + 1) * cols, :].astype(F32) for m in range(blocks)], axis=0)
            query = piece[:, :HEAD_DIM].astype(BF16)
            keys = piece[:, HEAD_DIM : 2 * HEAD_DIM].astype(BF16)
            weights = jnp.exp(dot_t(query, keys) + bias).astype(BF16)
            summed = dot(weights, jnp.where(lane < 3 * HEAD_DIM, piece, 1.0).astype(BF16))
            ratio = summed / roll(summed, -HEAD_DIM)
            group = a % 4
            inside = (lane >= group * HEAD_DIM) & (lane < (group + 1) * HEAD_DIM)
            slab = jnp.where(inside, roll(ratio, (group - 2) * HEAD_DIM), slab)
            if a == full - 1:
                for m in range(blocks):
                    send_ref[m, :cols, :] = slab[m * cols : (m + 1) * cols].astype(BF16)
                slab = jnp.zeros((length, LANES), F32)
        moved = roll(slab, 2 * HEAD_DIM)
        moved_on = roll(slab, HEAD_DIM)
        lane = lane_index(8)
        third = (lane >= 2 * HEAD_DIM) & (lane < 3 * HEAD_DIM)
        for m in range(blocks):
            low = m * cols
            tail = low + whole_rows
            out = jnp.concatenate(
                [
                    jnp.where(third, moved[tail : tail + 8], slab[low : low + 8]),
                    jnp.where(third, moved_on[tail : tail + 8], slab[low + 8 : tail]),
                ],
                axis=0,
            )
            send_ref[m, cols:, :] = out.astype(BF16)

    return attend


def finish_kernel(rows, cols, items):
    whole_rows = 16

    def finish(back_ref, gating_ref, after_ref, att_out_ref, out_ref):
        lane = lane_index(cols)
        pieces = []
        for a in range(rows):
            group, item = a // items, a % items
            mixed = jnp.zeros((cols, LANES), F32)
            for h in range(HEADS):
                block = h * (rows // items) + group
                if item < 4:
                    part = roll(back_ref[block, :cols, :].astype(F32), (h - item) * HEAD_DIM)
                else:
                    late = back_ref[block, cols:, :].astype(F32)
                    last = late[(item - 4) * 8 : (item - 3) * 8]
                    part = jnp.concatenate(
                        [roll(late, (h - item + 4) * HEAD_DIM), roll(last, (h - 2) * HEAD_DIM)], axis=0
                    )
                inside = (lane >= h * HEAD_DIM) & (lane < (h + 1) * HEAD_DIM)
                mixed = jnp.where(inside, part, mixed)
            pieces.append(mixed)
        attended = jnp.concatenate(pieces, axis=0)
        outgoing = (attended * gating_ref[...]).astype(BF16)
        out_ref[...] = (after_ref[...].astype(F32) + dot(outgoing, att_out_ref[...])).astype(BF16)

    return finish


def on_device(
    pair, chain_ids, residue_mask, chain_vec, tri_in, tri_gate, tri_out, att_query, att_kv, att_bias, att_out
):
    rows, cols, channels = pair.shape
    nrow, ncol, nsub = lax.axis_size("row"), lax.axis_size("col"), lax.axis_size("sub")
    positions = rows * cols
    length = chain_ids.shape[0]
    blocks = ncol * nsub
    items = HEADS * rows // blocks
    per_tile = LANES // cols
    tiles = -(-rows // per_tile)
    place = jnp.stack([lax.axis_index("row") * rows, lax.axis_index(("col", "sub")) * cols, lax.axis_index("sub")]).astype(jnp.int32)
    flat = pair.reshape(positions, channels)
    vec = chain_vec.reshape(1, channels)
    common = (flat, chain_ids, residue_mask, place, vec)

    (send,) = call(
        sides_kernel(rows, cols, per_tile, tiles),
        [((channels, 2 * tiles * LANES), BF16)],
        (place,) + tuple(in_hbm(x) for x in (flat, chain_ids, residue_mask, vec, tri_in)),
        "shhhhh",
        scratch=[
            pltpu.VMEM(flat.shape, flat.dtype),
            pltpu.SMEM(chain_ids.shape, jnp.int32),
            pltpu.SMEM(residue_mask.shape, jnp.int32),
            pltpu.VMEM(vec.shape, F32),
            pltpu.VMEM(tri_in.shape, tri_in.dtype),
        ]
        + [pltpu.SemaphoreType.DMA] * 5,
    )
    moved = lax.all_to_all(send.reshape(channels, 2, tiles * LANES), ("col", "row"), split_axis=0, concat_axis=0, tiled=True)
    bias_rows = jnp.pad(att_bias.T, ((0, 8 - HEADS), (0, 0)))
    start, tri_gating, head_weights, near_out, wide_bias = call(
        gate_kernel(rows, cols),
        [
            ((positions, channels), F32),
            ((positions, channels), F32),
            ((channels, HEADS * LANES), BF16),
            (tri_out.shape, BF16),
            ((channels, LANES), BF16),
        ],
        common + (tri_gate, att_query, att_kv, tri_out, bias_rows),
        "vsssvvvvvv",
    )
    live, start = lax.optimization_barrier((residue_mask.astype(F32).reshape(1, length), start))
    gathered = lax.all_gather(moved.reshape(channels, 2 * tiles * LANES), "sub", axis=0, tiled=True)
    (products,) = call(
        product_kernel(rows, cols, nrow, ncol, nsub, per_tile, tiles),
        [((nrow * ncol, rows // 4 * LANES), BF16)],
        (place, gathered),
        "sv",
        scratch=[
            pltpu.VMEM((length, blocks // 4 * LANES), BF16),
            pltpu.VMEM((blocks // 4 * length, LANES), F32),
        ],
    )
    returned = lax.all_to_all(products.reshape(nrow * ncol, 2, rows // 8 * LANES), ("col", "row"), split_axis=0, concat_axis=0, tiled=True)
    after, second, copies = call(
        after_kernel(rows, cols, nrow),
        [((positions, channels), BF16), ((positions, channels), BF16), ((nrow, rows, LANES), BF16)],
        (returned.reshape(channels, rows // 4 * LANES), start, tri_gating, near_out, wide_bias),
        "vvvvv",
    )
    plain_items, gating = call(
        items_kernel(positions),
        [((HEADS * positions, LANES), BF16), ((positions, channels), F32)],
        (second, head_weights, att_query),
        "vvv",
    )
    copies, plain_items, gating = lax.optimization_barrier((copies, plain_items, gating))
    columns = lax.all_to_all(copies, "row", split_axis=0, concat_axis=0, tiled=True)
    chunk = items * cols
    (sent_items,) = call(
        pack_kernel(chunk, cols, length, nsub),
        [((HEADS * positions, LANES), BF16)],
        (plain_items, columns.reshape(length, LANES)),
        "vv",
    )
    whole = lax.all_to_all(sent_items.reshape(blocks, chunk, LANES), ("col", "sub"), split_axis=0, concat_axis=0, tiled=True)
    (table_part,) = call(table_kernel(chunk, cols, blocks, length, nsub), [((length // nsub, length), BF16)], (whole,), "v")
    head_table = lax.all_gather(table_part, "sub", axis=0, tiled=True)
    (attended,) = call(
        attend_kernel(items, cols, blocks), [((blocks, cols + 16, LANES), BF16)], (whole, head_table, live), "vvv"
    )
    back = lax.all_to_all(attended, ("col", "sub"), split_axis=0, concat_axis=0, tiled=True)
    (result,) = call(
        finish_kernel(rows, cols, items), [((positions, channels), BF16)], (back, gating, after, att_out), "vvvv"
    )
    return result.reshape(rows, cols, channels)


def solution(mesh):
    return jax.shard_map(
        on_device,
        mesh=mesh,
        in_specs=(P(("grp", "row"), ("col", "sub"), None), P("grp"), P("grp")) + (P(),) * 8,
        out_specs=P(("grp", "row"), ("col", "sub"), None),
        check_vma=False,
    )
```
